128 devices in a mesh: rows: 16 (over x, z_lo, core), planes: 8 (over y, z_hi).
Axes of the slice: x: 4, y: 4, z: 4 (z_hi: 2, z_lo: 2; z = z_hi * 2 + z_lo), core: 2. Of those that a mesh axis runs over, the one named last changes fastest.
Arguments:
- density: float32 [8, 4096, 4096], P('planes', 'rows'), may hold values from -6 to 6
- lens_weight: float32 [8], P('planes'), may hold values from 0.05 to 0.5
- spectrum_bin: int32 [4096, 4096], P(None, ('rows', 'planes')), may hold values from 0 to 63, as said below
Outputs:
- shear_real: float32 [4096, 4096], P(('rows', 'planes'))
- shear_imag: float32 [4096, 4096], P(('rows', 'planes'))
- spectrum: float32 [64], replicated
The draws below stay inside these ranges and needn't reach their ends.
Inputs may be any that keep to these rules, and one draw needn't show every extreme that they name: `spectrum_bin`: each Fourier pixel's band.
All inputs are finite; a program needn't handle non-finite values.
Results may differ from the reference program's by a relative error of at most 0.0003.
Values sent between devices are 32-bit elements; how exact they have to be, the bound alone decides.
A program may use at most 64 MiB of HBM per device.

```python
import math
import jax
import jax.numpy as jnp
from jax import lax

N = 4096
NBINS = 64
PLANES = 8


def draw_spectrum_bin(key, part):
    frequency = (jnp.arange(N, dtype=jnp.int32) + N // 2) % N - N // 2
    square_norm = frequency[:, None] ** 2 + frequency[None, :] ** 2
    radial = jnp.minimum(square_norm * NBINS // (N * N // 2), NBINS - 1)
    jitter = jax.random.randint(key, (N, N), -1, 2, dtype=jnp.int32)
    return jnp.clip(radial + jitter, 0, NBINS - 1).astype(jnp.int32)


def level_of(rng, shape, cuts, least, high):
    level = 1.0
    for axis_at, parts in cuts:
        draws = jax.random.uniform(jax.random.fold_in(jax.random.fold_in(rng, 6), axis_at), (parts,), jnp.float32, least / len(cuts), high / len(cuts))
        level = level * jnp.repeat(jnp.exp(draws), shape[axis_at] // parts).reshape((-1,) + (1,) * (len(shape) - 1 - axis_at))
    return level


def bell_draw(rng, dims, spread, limit, cuts=(), held_as=jnp.bfloat16):
    entries = spread * jax.random.normal(rng, dims, jnp.float32)
    if cuts:
        entries = entries * level_of(rng, dims, cuts, -0.22, 0.18)
    return jnp.clip(entries, -limit, limit).astype(held_as)


def setup_inputs(seed: int = 0) -> dict:
    keys = jax.random.split(jax.random.key(seed), 4)
    return {
        "density": bell_draw(keys[0], (PLANES, N, N), 1.0, 6.0, ((0, 8), (1, 16)), jnp.float32),
        "lens_weight": jnp.clip(jnp.exp(math.log(0.5) - 2.3025851 * jax.random.uniform(keys[1], (PLANES,), jnp.float32) ** level_of(keys[1], (PLANES,), ((0, 8),), -0.2, 0.2)), 0.05, 0.5),
        "spectrum_bin": draw_spectrum_bin(jax.random.fold_in(keys[3], 71), 0),
    }


def reference(density, lens_weight, spectrum_bin):
    def accumulate(plane_index, running):
        total_real, total_imag = running
        weighted_plane = density[plane_index] * lens_weight[plane_index]
        plane_hat = jnp.fft.fft2(weighted_plane)
        return (total_real + jnp.real(plane_hat), total_imag + jnp.imag(plane_hat))

    empty_sum = jnp.zeros((N, N), jnp.float32)
    total_real, total_imag = lax.fori_loop(0, PLANES, accumulate, (empty_sum, empty_sum))
    frequency = ((jnp.arange(N, dtype=jnp.int32) + N // 2) % N - N // 2).astype(jnp.float32)
    height = frequency[:, None]
    across = frequency[None, :]
    square_norm = height ** 2 + across ** 2
    anchor = square_norm == 0
    safe_norm = jnp.where(anchor, 1.0, square_norm)
    total_real = jnp.where(anchor, 0.0, total_real)
    total_imag = jnp.where(anchor, 0.0, total_imag)
    pixel_power = (total_real ** 2 + total_imag ** 2) * (NBINS / float(N) ** 4)
    spectrum = jax.ops.segment_sum(pixel_power.reshape(-1), spectrum_bin.reshape(-1), num_segments=NBINS)
    kernel_real = (across ** 2 - height ** 2) / safe_norm
    kernel_imag = 2.0 * across * height / safe_norm
    hat_real = kernel_real * total_real - kernel_imag * total_imag
    hat_imag = kernel_real * total_imag + kernel_imag * total_real
    shear_field = jnp.fft.ifft2(hat_real + 1j * hat_imag)
    return jnp.real(shear_field).astype(jnp.float32), jnp.imag(shear_field).astype(jnp.float32), spectrum
```

```python
from functools import partial
import math

import jax
import jax.numpy as jnp
import ml_dtypes
import numpy as np
from jax import lax
from jax.experimental import pallas as pl
from jax.experimental.pallas import tpu as pltpu
from jax.sharding import Mesh
from jax.sharding import PartitionSpec as P

N = 4096
NBINS = 64
DEVICES = 128
AXES = ("x", "zl", "core", "y", "zh")
ROWS = ("x", "zl", "core")
PLANES = ("y", "zh")
LOGICAL = pl.DeviceIdType.LOGICAL
F32 = jnp.float32
BF16 = jnp.bfloat16


def halves(table):
    high = table.astype(np.float32).astype(ml_dtypes.bfloat16)
    low = (table - high.astype(np.float64)).astype(np.float32).astype(ml_dtypes.bfloat16)
    return np.stack([high, low])


def make_tables():
    turn = 2.0 * math.pi
    i128 = np.arange(128)
    angle = turn * ((i128[:, None] * i128[None, :]) % 128) / 128
    cos, sin = np.cos(angle), np.sin(angle)
    forward = np.block([[cos, sin], [-sin, cos]])
    inverse = np.block([[cos, -sin], [sin, cos]])
    first = np.zeros((256, 256))
    back = np.zeros((256, 256))
    for d in range(128):
        if d < 64:
            phase = turn * (((16 + 32 * d) * i128) % 4096) / 4096
            first[d, 128:] = np.cos(phase)
            first[128 + d, 128:] = -np.sin(phase)
            weight = 2.0
        elif d == 64:
            first[d, :128] = 1.0
            first[128 + d, :128] = (-1.0) ** i128
            weight = 1.0
        else:
            phase = turn * ((d * i128) % 128) / 128
            first[d, :128] = np.cos(phase)
            first[128 + d, :128] = -np.sin(phase)
            weight = 2.0
        back[:, d] = weight * first[d]
        back[:, 128 + d] = weight * first[128 + d]
    small = np.zeros((4, 32, 32, 4), np.complex128)
    i32 = np.arange(32)
    kernel = np.exp(-1j * turn * ((i32[:, None] * i32[None, :]) % 32) / 32)
    for c in range(4):
        small[c, :, :, c] = kernel
    small = small.reshape(128, 128)
    lanes = np.block([[small.real, small.imag], [-small.imag, small.real]])
    wide = np.conj(small).T
    lanes_back = np.block([[wide.real, wide.imag], [-wide.imag, wide.real]])
    mats = np.stack([halves(t) for t in (forward, inverse, first, back, lanes, lanes_back)])
    y2 = np.tile(i32, 4)
    phase = turn * (i128[:, None] * y2[None, :]) / 4096
    column_twiddle = np.stack([np.cos(phase), np.sin(phase)]).astype(np.float32)
    phase = turn * (np.arange(16)[:, None] * i128[None, :]) / 4096
    row_twiddle = np.stack([np.cos(phase), np.sin(phase)]).astype(np.float32)
    return mats, column_twiddle, row_twiddle


FORWARD, INVERSE, FIRST, BACK, LANES, LANES_BACK = range(6)


def rfft(values):
    n = len(values)
    if n == 2:
        return [(values[0] + values[1], None), (values[0] - values[1], None)]
    even, odd = rfft(values[0::2]), rfft(values[1::2])
    out = [None] * (n // 2 + 1)
    out[0] = (even[0][0] + odd[0][0], None)
    out[n // 2] = (even[0][0] - odd[0][0], None)
    for k in range(1, n // 4):
        c, s = math.cos(2 * math.pi * k / n), math.sin(2 * math.pi * k / n)
        er, ei = even[k]
        orr, oi = odd[k]
        if 8 * k == n:
            pr, pi = (orr + oi) * c, (oi - orr) * c
        else:
            pr, pi = orr * c + oi * s, oi * c - orr * s
        out[k] = (er + pr, ei + pi)
        out[n // 2 - k] = (er - pr, pi - ei)
    out[n // 4] = (even[n // 4][0], -odd[n // 4][0])
    return out


def irfft(g):
    n = 2 * (len(g) - 1)
    if n == 2:
        return [g[0][0] + g[1][0], g[0][0] - g[1][0]]
    even, odd = [None] * (n // 4 + 1), [None] * (n // 4 + 1)
    even[0] = (g[0][0] + g[n // 2][0], None)
    odd[0] = (g[0][0] - g[n // 2][0], None)
    for k in range(1, n // 4):
        c, s = math.cos(2 * math.pi * k / n), math.sin(2 * math.pi * k / n)
        ar, ai = g[k]
        br, bi = g[n // 2 - k]
        even[k] = (ar + br, ai - bi)
        dr, di = ar - br, ai + bi
        odd[k] = (dr * c - di * s, dr * s + di * c)
    mr, mi = g[n // 4]
    even[n // 4] = (mr + mr, None)
    odd[n // 4] = (-(mi + mi), None)
    a, b = irfft(even), irfft(odd)
    out = [None] * n
    out[0::2], out[1::2] = a, b
    return out


def split(value):
    high = value.astype(BF16)
    return high, (value - high.astype(F32)).astype(BF16)


def table_times(mats, which, data):
    high, low = split(data)
    dot = partial(jnp.dot, preferred_element_type=F32)
    return dot(mats[which, 0], high) + dot(mats[which, 0], low) + dot(mats[which, 1], high)


def times_table(mats, which, data):
    high, low = split(data)
    dot = partial(jnp.dot, preferred_element_type=F32)
    return dot(high, mats[which, 0]) + dot(low, mats[which, 0]) + dot(high, mats[which, 1])


def my_index():
    x, zl, core, y, zh = (lax.axis_index(a) for a in AXES)
    return ((x * 2 + zl) * 2 + core) * 8 + y * 2 + zh


def row_forward(res, mats, rtw, ubuf, msg):
    for q in range(4):
        rows = pl.ds(q * 8, 8)
        out = rfft([res[rows, pl.ds(x1 * 128, 128)] for x1 in range(32)])
        for k1 in range(16):
            at = pl.ds(k1 * 32 + q * 8, 8)
            if k1 == 0:
                ubuf[0, at, :], ubuf[1, at, :] = out[0][0], out[16][0]
            else:
                tr, ti = rtw[0, pl.ds(k1, 1), :], rtw[1, pl.ds(k1, 1), :]
                ur, ui = out[k1]
                ubuf[0, at, :] = ur * tr + ui * ti
                ubuf[1, at, :] = ui * tr - ur * ti
    data = jnp.concatenate([ubuf[0].T, ubuf[1].T], axis=0)
    spread = table_times(mats, FORWARD, data)
    special = table_times(mats, FIRST, data[:, :128])
    lane = lax.broadcasted_iota(jnp.int32, (256, 128), 1)
    for t in range(4):
        piece = spread[:, t * 128 : (t + 1) * 128]
        if t == 0:
            piece = jnp.where(lane < 32, special, piece)
        for c in range(2):
            msg[pl.ds(c * 4 + t, 128, stride=8), :] = piece[c * 128 : (c + 1) * 128]


def column_part(me, recv, mats, ctw, power, msg):
    lane = lax.broadcasted_iota(jnp.int32, (128, 128), 1)
    sub = lax.broadcasted_iota(jnp.int32, (128, 128), 0)
    special = jnp.logical_and(lane < 32, me == 64)
    re = [recv[pl.ds(t, 128, stride=8), :] for t in range(4)]
    im = [recv[pl.ds(4 + t, 128, stride=8), :] for t in range(4)]
    zero = jnp.zeros((128, 128), F32)
    re.append(jnp.where(special, im[0], zero))
    im[0] = jnp.where(special, zero, im[0])
    im.append(zero)
    data = jnp.concatenate([jnp.concatenate(re, axis=1), jnp.concatenate(im, axis=1)], axis=0)
    y = table_times(mats, FORWARD, data)
    tc, ts = ctw[0], ctw[1]
    rows = []
    for t in range(5):
        yr, yi = y[:128, t * 128 : (t + 1) * 128], y[128:, t * 128 : (t + 1) * 128]
        rows.append(jnp.concatenate([yr * tc + yi * ts, yi * tc - yr * ts], axis=1))
    f = times_table(mats, LANES, jnp.concatenate(rows, axis=0))
    ky2 = lane // 4
    col = lane % 4
    ky = sub + 128 * ky2
    nyquist = ky == 2048
    ky = jnp.where(ky >= 2048, ky - 4096, ky).astype(F32)
    scale = 1.0 / (float(N) * float(N))
    hats = []
    for t in range(5):
        fr, fi = f[t * 128 : (t + 1) * 128, :128], f[t * 128 : (t + 1) * 128, 128:]
        if t < 4:
            slot = t * 4 + col
            kx = slot + 32 * me
            if t == 0:
                zeroth = jnp.where(
                    me < 64, 16 + 32 * me, jnp.where(me == 64, 0, 32 * me)
                )
                kx = jnp.where(slot == 0, zeroth, kx)
            kx = jnp.where(kx >= 2048, kx - 4096, kx).astype(F32)
        else:
            kx = jnp.full((128, 128), -2048.0, F32)
        norm = kx * kx + ky * ky
        if t == 0:
            anchor = norm == 0
            norm = jnp.where(anchor, 1.0, norm)
            fr, fi = jnp.where(anchor, 0.0, fr), jnp.where(anchor, 0.0, fi)
        power[t] = fr * fr + fi * fi
        inv = scale / norm
        kr = (kx * kx - ky * ky) * inv
        ki = 2.0 * kx * ky * inv
        if t < 4:
            kn = jnp.where(nyquist, ki, 0.0)
            ki = jnp.where(nyquist, 0.0, ki)
            a = (kr * fr - kn * fi, kr * fi + kn * fr)
            c = (ki * fr, ki * fi)
        else:
            kn = jnp.where(nyquist, ki, 0.0)
            ki = jnp.where(nyquist, 0.0, ki)
            a = (kr * fr - ki * fi, kr * fi + ki * fr)
            c = (kn * fr, kn * fi)
        hats.append((a, c))
    rows = [jnp.concatenate(hats[t][ac], axis=1) for ac in range(2) for t in range(5)]
    g = times_table(mats, LANES_BACK, jnp.concatenate(rows, axis=0))
    re, im = [], []
    for i in range(10):
        gr, gi = g[i * 128 : (i + 1) * 128, :128], g[i * 128 : (i + 1) * 128, 128:]
        re.append(gr * tc - gi * ts)
        im.append(gi * tc + gr * ts)
    data = jnp.concatenate([jnp.concatenate(re, axis=1), jnp.concatenate(im, axis=1)], axis=0)
    s = table_times(mats, INVERSE, data)
    for ac in range(2):
        for t in range(4):
            at = (ac * 5 + t) * 128
            sr, si = s[:128, at : at + 128], s[128:, at : at + 128]
            if t == 0:
                extra = (ac * 5 + 4) * 128
                si = jnp.where(special, s[:128, extra : extra + 128], si)
            msg[pl.ds(ac * 8 + t, 128, stride=16), :] = sr
            msg[pl.ds(ac * 8 + 4 + t, 128, stride=16), :] = si


def row_inverse(recv, mats, rtw, vbuf, outs):
    lane = lax.broadcasted_iota(jnp.int32, (256, 128), 1)
    for ac in range(2):
        parts = [
            jnp.concatenate(
                [recv[pl.ds(ac * 8 + c * 4 + t, 128, stride=16), :] for t in range(4)], axis=1
            )
            for c in range(2)
        ]
        data = jnp.concatenate(parts, axis=0)
        v = table_times(mats, INVERSE, data)
        special = table_times(mats, BACK, data[:, :128])
        first = jnp.where(lane < 32, special, v[:, :128])
        for c in range(2):
            rows = slice(c * 128, (c + 1) * 128)
            full = jnp.concatenate([first[rows], v[rows, 128:]], axis=1)
            vbuf[c] = full.T
        for q in range(4):
            g = [None] * 17
            for k1 in range(16):
                at = pl.ds(k1 * 32 + q * 8, 8)
                vr, vi = vbuf[0, at, :], vbuf[1, at, :]
                if k1 == 0:
                    g[0], g[16] = (vr, None), (vi, None)
                else:
                    tr, ti = rtw[0, pl.ds(k1, 1), :], rtw[1, pl.ds(k1, 1), :]
                    g[k1] = (vr * tr - vi * ti, vi * tr + vr * ti)
            out = irfft(g)
            for x1 in range(32):
                outs[ac][pl.ds(q * 8, 8), pl.ds(x1 * 128, 128)] = out[x1]


def send_all(me, msg, recv, send, arrive, rows):
    def step(i, _):
        to = lax.rem(me + i, DEVICES)
        pltpu.make_async_remote_copy(
            src_ref=msg.at[pl.ds(pl.multiple_of(to * rows, rows), rows)],
            dst_ref=recv.at[pl.ds(pl.multiple_of(me * rows, rows), rows)],
            send_sem=send,
            recv_sem=arrive,
            device_id=to,
            device_id_type=LOGICAL,
        ).start()
        return 0

    lax.fori_loop(1, DEVICES, step, 0)
    own = pl.ds(pl.multiple_of(me * rows, rows), rows)
    recv[own, :] = msg[own, :]


def wait_all(buf, sem, rows):
    part = buf.at[pl.ds(0, (DEVICES - 1) * rows)]
    pltpu.make_async_copy(part, part, sem).wait()


def bin_power(bins, power, acc, spec):
    def group(g, _):
        sums = [jnp.zeros((8, 128), F32) for _ in range(8)]
        for i in range(9):
            t = i % 5 if i < 5 else i - 5
            which = 0 if i < 5 else 1
            for r in range(16):
                at = pl.ds(r * 8, 8)
                b = bins[which, t, at, :] - g * 8
                p = power[t, at, :]
                for k in range(8):
                    sums[k] = sums[k] + jnp.where(b == k, p, 0.0)
        rows = [jnp.sum(v, axis=0, keepdims=True) for v in sums]
        acc[pl.ds(pl.multiple_of(g * 8, 8), 8), :] = jnp.concatenate(rows, axis=0)
        return 0

    lax.fori_loop(0, 8, group, 0)
    acc[pl.ds(64, 64), :] = jnp.zeros((64, 128), F32)
    row = jnp.sum(acc[...].T, axis=0, keepdims=True)
    spec[0] = row * (NBINS / float(N) ** 4)


def reduce_planes(weight, mine, res, yf, zf, yrelay, ydirect, yfinal, zrecv, zsum, ssem, rsem):
    y, zh = lax.axis_index("y"), lax.axis_index("zh")
    base = my_index() - y * 2 - zh
    up, down, across = lax.rem(y + 1, 4), lax.rem(y + 3, 4), lax.rem(y + 2, 4)
    dev_up, dev_down = base + up * 2 + zh, base + down * 2 + zh
    dev_z = base + y * 2 + (1 - zh)
    count = [0]
    sends = []

    def send(src, dst, to):
        i = count[0]
        count[0] += 1
        copy = pltpu.make_async_remote_copy(
            src_ref=src,
            dst_ref=dst,
            send_sem=ssem.at[i],
            recv_sem=rsem.at[i],
            device_id=to,
            device_id_type=LOGICAL,
        )
        copy.start()
        sends.append(copy)
        return copy

    def share(t, h, q):
        return mine.at[pl.ds(pl.multiple_of((t * 2 + h) * 32 + q * 8, 8), 8)]

    znew = {}
    for q in zf:
        for i, t in enumerate((across, up, down, y)):
            znew[q, i] = send(share(t, 1 - zh, q), zrecv.at[q, i], dev_z)
    relay, direct, final = {}, {}, {}
    for q in yf:
        relay[q, 0] = send(share(across, 0, q), yrelay.at[q, 0], dev_up)
        relay[q, 1] = send(share(across, 1, q), yrelay.at[q, 1], dev_down)
        direct[q, 0] = send(share(up, 1, q), ydirect.at[q, 1], dev_up)
        direct[q, 1] = send(share(down, 0, q), ydirect.at[q, 0], dev_down)
    half = (slice(0, 2048), slice(2048, 4096))

    def y_relay_first(q):
        relay[q, 0].wait_recv()
        yrelay[q, 0] = yrelay[q, 0] + share(up, 0, q)[...]
        final[q, 0] = send(yrelay.at[q, 0], yfinal.at[q, 0], dev_up)
        relay[q, 1].wait_recv()
        yrelay[q, 1] = yrelay[q, 1] + share(down, 1, q)[...]
        final[q, 1] = send(yrelay.at[q, 1], yfinal.at[q, 1], dev_down)

    def y_finish_first(q):
        for h in range(2):
            direct[q, h].wait_recv()
            final[q, h].wait_recv()
        for h in range(2):
            yfinal[q, h] = yfinal[q, h] + ydirect[q, h] + share(y, h, q)[...]
        znew[q, 0] = send(yfinal.at[q, 1 - zh], zrecv.at[q, 0], dev_z)

    def z_last(q):
        znew[q, 0].wait_recv()
        res[pl.ds(q * 8, 8), :] = zrecv[q, 0] + yfinal[q, zh]

    def z_first(q):
        for i, t in enumerate((across, up, down, y)):
            znew[q, i].wait_recv()
            zsum[q, i] = zrecv[q, i] + share(t, zh, q)[...]
            if i == 0:
                relay[q, 0] = send(
                    zsum.at[q, 0, :, pl.ds(0, 2048)], yrelay.at[q, 0, :, pl.ds(0, 2048)], dev_up
                )
                relay[q, 1] = send(
                    zsum.at[q, 0, :, pl.ds(2048, 2048)], yrelay.at[q, 1, :, pl.ds(0, 2048)], dev_down
                )
            if i == 1:
                direct[q, 0] = send(
                    zsum.at[q, 1, :, pl.ds(2048, 2048)], ydirect.at[q, 1, :, pl.ds(0, 2048)], dev_up
                )
            if i == 2:
                direct[q, 1] = send(
                    zsum.at[q, 2, :, pl.ds(0, 2048)], ydirect.at[q, 0, :, pl.ds(0, 2048)], dev_down
                )

    def y_relay_last(q):
        relay[q, 0].wait_recv()
        yrelay[q, 0, :, :2048] = yrelay[q, 0, :, :2048] + zsum[q, 1, :, half[0]]
        final[q, 0] = send(
            yrelay.at[q, 0, :, pl.ds(0, 2048)], yfinal.at[q, 0, :, pl.ds(0, 2048)], dev_up
        )
        relay[q, 1].wait_recv()
        yrelay[q, 1, :, :2048] = yrelay[q, 1, :, :2048] + zsum[q, 2, :, half[1]]
        final[q, 1] = send(
            yrelay.at[q, 1, :, pl.ds(0, 2048)], yfinal.at[q, 1, :, pl.ds(0, 2048)], dev_down
        )

    def y_last(q):
        for h in range(2):
            direct[q, h].wait_recv()
            final[q, h].wait_recv()
        for h in range(2):
            res[pl.ds(q * 8, 8), half[h]] = (
                zsum[q, 3, :, half[h]] + yfinal[q, h, :, :2048] + ydirect[q, h, :, :2048]
            )

    y_relay_first(yf[0])
    y_relay_first(yf[1])
    y_finish_first(yf[0])
    z_first(zf[0])
    y_relay_last(zf[0])
    y_finish_first(yf[1])
    z_first(zf[1])
    y_relay_last(zf[1])
    y_last(zf[0])
    z_last(yf[0])
    z_last(yf[1])
    y_last(zf[1])
    return sends


def kernel(
    density, weight, bins, mats_in, ctw, rtw, out_real, out_imag, out_spec,
    mine, res, mats, yrelay, ydirect, yfinal, zrecv, zsum,
    ubuf, msgb, recvb, msgc, recvc, power, acc, spec, specs,
    lsem, msem, ssem, rsem, asem,
):
    me = my_index()
    barrier = pltpu.get_barrier_semaphore()
    loads = []
    for i in range(8):
        copy = pltpu.make_async_copy(
            density.at[0, pl.ds(i * 32, 32)], mine.at[pl.ds(i * 32, 32)], lsem.at[i]
        )
        copy.start()
        loads.append(copy)
    mload = pltpu.make_async_copy(mats_in, mats, msem)
    mload.start()

    def greet(i, _):
        pl.semaphore_signal(
            barrier, inc=1, device_id=lax.rem(me + i, DEVICES), device_id_type=LOGICAL
        )
        return 0

    lax.fori_loop(1, DEVICES, greet, 0)
    w = weight[0]
    for i in range(8):
        loads[i].wait()
        rows = pl.ds(i * 32, 32)
        mine[rows, :] = mine[rows, :] * w
    pl.semaphore_wait(barrier, DEVICES - 1)
    sends = reduce_planes(
        weight, mine, res, (0, 1), (2, 3), yrelay, ydirect, yfinal, zrecv, zsum, ssem, rsem
    )
    mload.wait()
    row_forward(res, mats, rtw, ubuf, msgb)
    send_all(me, msgb, recvb, asem.at[0], asem.at[1], 8)
    wait_all(recvb, asem.at[1], 8)
    column_part(me, recvb, mats, ctw, power, msgc)
    send_all(me, msgc, recvc, asem.at[2], asem.at[3], 16)
    bin_power(bins, power, acc, spec)

    def share_spec(i, _):
        to = lax.rem(me + i, DEVICES)
        pltpu.make_async_remote_copy(
            src_ref=spec.at[0],
            dst_ref=specs.at[me],
            send_sem=asem.at[4],
            recv_sem=asem.at[5],
            device_id=to,
            device_id_type=LOGICAL,
        ).start()
        return 0

    lax.fori_loop(1, DEVICES, share_spec, 0)
    specs[me] = spec[0]
    wait_all(recvc, asem.at[3], 16)
    row_inverse(recvc, mats, rtw, ubuf, (out_real, out_imag))
    wait_all(specs, asem.at[5], 1)
    total = specs[0]
    for i in range(1, DEVICES):
        total = total + specs[i]
    out_spec[...] = total
    wait_all(msgb, asem.at[0], 8)
    wait_all(msgc, asem.at[2], 16)
    wait_all(specs, asem.at[4], 1)
    for copy in sends:
        copy.wait_send()


def bin_tables(me, raw):
    pairs = [(d, 127 - d) for d in range(DEVICES)]
    mirrored = lax.ppermute(raw[:, 16:], AXES, pairs)
    single = jnp.where(me < 64, raw[:, 0], raw[:, 16])
    pairs = [(d, (64 if d == 0 else 128 - d) if d < 64 else 127 - d) for d in range(DEVICES)]
    extra = lax.ppermute(single, AXES, pairs)
    first = jnp.where(me < 64, raw[:, 16], jnp.where(me == 64, NBINS, raw[:, 0]))
    near = jnp.concatenate([first[:, None], raw[:, 1:16]], axis=1)
    far = jnp.concatenate([extra[:, None], mirrored[:, :0:-1]], axis=1)
    far = jnp.concatenate([far[:1], far[:0:-1]], axis=0)
    last = jnp.concatenate([raw[:, :1], jnp.full((N, 3), NBINS, jnp.int32)], axis=1)

    def arranged(cols):
        tiles = cols.shape[1] // 4
        return cols.reshape(32, 128, tiles, 4).transpose(2, 1, 0, 3).reshape(tiles, 128, 128)

    near = arranged(jnp.concatenate([near, last], axis=1))
    far = jnp.concatenate([arranged(far), jnp.full((1, 128, 128), NBINS, jnp.int32)], axis=0)
    return jnp.stack([near, far])


def on_device(tables, density, lens_weight, spectrum_bin):
    mats, ctw, rtw = tables
    bins = bin_tables(my_index(), spectrum_bin)
    vmem = pl.BlockSpec(memory_space=pltpu.VMEM)
    hbm = pl.BlockSpec(memory_space=pl.ANY)
    smem = pl.BlockSpec(memory_space=pltpu.SMEM)
    dma = pltpu.SemaphoreType.DMA
    share = (8, 4096)
    out = pl.pallas_call(
        kernel,
        name="shear",
        out_shape=(
            jax.ShapeDtypeStruct((32, N), F32),
            jax.ShapeDtypeStruct((32, N), F32),
            jax.ShapeDtypeStruct((1, 128), F32),
        ),
        in_specs=[hbm, smem, vmem, hbm, vmem, vmem],
        out_specs=(vmem, vmem, vmem),
        scratch_shapes=[
            pltpu.VMEM((256, N), F32),
            pltpu.VMEM((32, N), F32),
            pltpu.VMEM((6, 2, 256, 256), BF16),
            pltpu.VMEM((4, 2) + share, F32),
            pltpu.VMEM((4, 2) + share, F32),
            pltpu.VMEM((4, 2) + share, F32),
            pltpu.VMEM((4, 4) + share, F32),
            pltpu.VMEM((4, 4) + share, F32),
            pltpu.VMEM((2, 512, 128), F32),
            pltpu.VMEM((DEVICES * 8, 128), F32),
            pltpu.VMEM((DEVICES * 8, 128), F32),
            pltpu.VMEM((DEVICES * 16, 128), F32),
            pltpu.VMEM((DEVICES * 16, 128), F32),
            pltpu.VMEM((5, 128, 128), F32),
            pltpu.VMEM((128, 128), F32),
            pltpu.VMEM((1, 1, 128), F32),
            pltpu.VMEM((DEVICES, 1, 128), F32),
            dma((8,)),
            dma,
            dma((40,)),
            dma((40,)),
            dma((6,)),
        ],
        compiler_params=pltpu.CompilerParams(
            collective_id=0, has_side_effects=True, vmem_limit_bytes=60 * 1024 * 1024
        ),
    )(density, lens_weight, bins, mats, ctw, rtw)
    return out[0], out[1], out[2][0, :NBINS]


def solution(mesh):
    finer = Mesh(mesh.devices.reshape(4, 2, 2, 4, 2), AXES)
    tables = tuple(jnp.asarray(t) for t in make_tables())
    step = jax.shard_map(
        partial(on_device),
        mesh=finer,
        in_specs=((P(), P(), P()), P(PLANES, ROWS, None), P(PLANES), P(None, AXES)),
        out_specs=(P(AXES, None), P(AXES, None), P()),
        check_vma=False,
    )

    def whole(density, lens_weight, spectrum_bin):
        return step(tables, density, lens_weight, spectrum_bin)

    return whole
```

```python
from functools import partial
import math

import jax
import jax.numpy as jnp
import ml_dtypes
import numpy as np
from jax import lax
from jax.experimental import pallas as pl
from jax.experimental.pallas import tpu as pltpu
from jax.sharding import Mesh
from jax.sharding import PartitionSpec as P

N = 4096
NBINS = 64
DEVICES = 128
AXES = ("x", "zl", "core", "y", "zh")
ROWS = ("x", "zl", "core")
PLANES = ("y", "zh")
LOGICAL = pl.DeviceIdType.LOGICAL
F32 = jnp.float32
BF16 = jnp.bfloat16


def halves(table):
    high = table.astype(np.float32).astype(ml_dtypes.bfloat16)
    low = (table - high.astype(np.float64)).astype(np.float32).astype(ml_dtypes.bfloat16)
    return np.stack([high, low])


def make_tables():
    turn = 2.0 * math.pi
    i128 = np.arange(128)
    angle = turn * ((i128[:, None] * i128[None, :]) % 128) / 128
    cos, sin = np.cos(angle), np.sin(angle)
    forward = np.block([[cos, sin], [-sin, cos]])
    inverse = np.block([[cos, -sin], [sin, cos]])
    first = np.zeros((256, 256))
    back = np.zeros((256, 256))
    for d in range(128):
        if d < 64:
            phase = turn * (((16 + 32 * d) * i128) % 4096) / 4096
            first[d, 128:] = np.cos(phase)
            first[128 + d, 128:] = -np.sin(phase)
            weight = 2.0
        elif d == 64:
            first[d, :128] = 1.0
            first[128 + d, :128] = (-1.0) ** i128
            weight = 1.0
        else:
            phase = turn * ((d * i128) % 128) / 128
            first[d, :128] = np.cos(phase)
            first[128 + d, :128] = -np.sin(phase)
            weight = 2.0
        back[:, d] = weight * first[d]
        back[:, 128 + d] = weight * first[128 + d]
    small = np.zeros((4, 32, 32, 4), np.complex128)
    i32 = np.arange(32)
    kernel = np.exp(-1j * turn * ((i32[:, None] * i32[None, :]) % 32) / 32)
    for c in range(4):
        small[c, :, :, c] = kernel
    small = small.reshape(128, 128)
    lanes = np.block([[small.real, small.imag], [-small.imag, small.real]])
    wide = np.conj(small).T
    lanes_back = np.block([[wide.real, wide.imag], [-wide.imag, wide.real]])
    mats = np.stack([halves(t) for t in (forward, inverse, first, back, lanes, lanes_back)])
    y2 = np.tile(i32, 4)
    phase = turn * (i128[:, None] * y2[None, :]) / 4096
    column_twiddle = np.stack([np.cos(phase), np.sin(phase)]).astype(np.float32)
    phase = turn * (np.arange(16)[:, None] * i128[None, :]) / 4096
    row_twiddle = np.stack([np.cos(phase), np.sin(phase)]).astype(np.float32)
    extra = np.zeros((1, 2, 256, 256), ml_dtypes.bfloat16)
    for c in range(2):
        for j, (up, left) in enumerate(((0, 0), (0, 128), (128, 0))):
            part = column_twiddle[c].astype(ml_dtypes.bfloat16)
            column_twiddle[c] -= part.astype(np.float32)
            extra[0, c, up : up + 128, left : left + 128] = part
            part = row_twiddle[c].astype(ml_dtypes.bfloat16)
            row_twiddle[c] -= part.astype(np.float32)
            extra[0, c, 128 + 16 * j : 144 + 16 * j, 128:] = part
    return np.concatenate([mats, extra])


FORWARD, INVERSE, FIRST, BACK, LANES, LANES_BACK, TWIDDLES = range(7)


def rfft(values):
    n = len(values)
    if n == 2:
        return [(values[0] + values[1], None), (values[0] - values[1], None)]
    even, odd = rfft(values[0::2]), rfft(values[1::2])
    out = [None] * (n // 2 + 1)
    out[0] = (even[0][0] + odd[0][0], None)
    out[n // 2] = (even[0][0] - odd[0][0], None)
    for k in range(1, n // 4):
        c, s = math.cos(2 * math.pi * k / n), math.sin(2 * math.pi * k / n)
        er, ei = even[k]
        orr, oi = odd[k]
        if 8 * k == n:
            pr, pi = (orr + oi) * c, (oi - orr) * c
        else:
            pr, pi = orr * c + oi * s, oi * c - orr * s
        out[k] = (er + pr, ei + pi)
        out[n // 2 - k] = (er - pr, pi - ei)
    out[n // 4] = (even[n // 4][0], -odd[n // 4][0])
    return out


def irfft(g):
    n = 2 * (len(g) - 1)
    if n == 2:
        return [g[0][0] + g[1][0], g[0][0] - g[1][0]]
    even, odd = [None] * (n // 4 + 1), [None] * (n // 4 + 1)
    even[0] = (g[0][0] + g[n // 2][0], None)
    odd[0] = (g[0][0] - g[n // 2][0], None)
    for k in range(1, n // 4):
        c, s = math.cos(2 * math.pi * k / n), math.sin(2 * math.pi * k / n)
        ar, ai = g[k]
        br, bi = g[n // 2 - k]
        even[k] = (ar + br, ai - bi)
        dr, di = ar - br, ai + bi
        odd[k] = (dr * c - di * s, dr * s + di * c)
    mr, mi = g[n // 4]
    even[n // 4] = (mr + mr, None)
    odd[n // 4] = (-(mi + mi), None)
    a, b = irfft(even), irfft(odd)
    out = [None] * n
    out[0::2], out[1::2] = a, b
    return out


def split(value):
    high = value.astype(BF16)
    return high, (value - high.astype(F32)).astype(BF16)


def table_times(mats, which, data):
    high, low = split(data)
    dot = partial(jnp.dot, preferred_element_type=F32)
    return dot(mats[which, 0], high) + dot(mats[which, 0], low) + dot(mats[which, 1], high)


def times_table(mats, which, data):
    high, low = split(data)
    dot = partial(jnp.dot, preferred_element_type=F32)
    return dot(high, mats[which, 0]) + dot(low, mats[which, 0]) + dot(high, mats[which, 1])


def read_twiddles(mats, ctw, rtw):
    for c in range(2):
        parts = [
            mats[TWIDDLES, c, pl.ds(up, 128), pl.ds(left, 128)].astype(F32)
            for up, left in ((0, 0), (0, 128), (128, 0))
        ]
        ctw[c] = parts[0] + parts[1] + parts[2]
        parts = [
            mats[TWIDDLES, c, pl.ds(128 + 16 * j, 16), pl.ds(128, 128)].astype(F32)
            for j in range(3)
        ]
        rtw[c] = parts[0] + parts[1] + parts[2]


def my_index():
    x, zl, core, y, zh = (lax.axis_index(a) for a in AXES)
    return ((x * 2 + zl) * 2 + core) * 8 + y * 2 + zh


def row_forward(res, mats, rtw, ubuf, msg):
    for q in range(4):
        rows = pl.ds(q * 8, 8)
        out = rfft([res[rows, pl.ds(x1 * 128, 128)] for x1 in range(32)])
        for k1 in range(16):
            at = pl.ds(k1 * 32 + q * 8, 8)
            if k1 == 0:
                ubuf[0, at, :], ubuf[1, at, :] = out[0][0], out[16][0]
            else:
                tr, ti = rtw[0, pl.ds(k1, 1), :], rtw[1, pl.ds(k1, 1), :]
                ur, ui = out[k1]
                ubuf[0, at, :] = ur * tr + ui * ti
                ubuf[1, at, :] = ui * tr - ur * ti
    data = jnp.concatenate([ubuf[0].T, ubuf[1].T], axis=0)
    spread = table_times(mats, FORWARD, data)
    special = table_times(mats, FIRST, data[:, :128])
    lane = lax.broadcasted_iota(jnp.int32, (256, 128), 1)
    for t in range(4):
        piece = spread[:, t * 128 : (t + 1) * 128]
        if t == 0:
            piece = jnp.where(lane < 32, special, piece)
        for c in range(2):
            msg[pl.ds(c * 4 + t, 128, stride=8), :] = piece[c * 128 : (c + 1) * 128]


def column_part(me, recv, mats, ctw, power, msg):
    lane = lax.broadcasted_iota(jnp.int32, (128, 128), 1)
    sub = lax.broadcasted_iota(jnp.int32, (128, 128), 0)
    special = jnp.logical_and(lane < 32, me == 64)
    re = [recv[pl.ds(t, 128, stride=8), :] for t in range(4)]
    im = [recv[pl.ds(4 + t, 128, stride=8), :] for t in range(4)]
    zero = jnp.zeros((128, 128), F32)
    re.append(jnp.where(special, im[0], zero))
    im[0] = jnp.where(special, zero, im[0])
    im.append(zero)
    data = jnp.concatenate([jnp.concatenate(re, axis=1), jnp.concatenate(im, axis=1)], axis=0)
    y = table_times(mats, FORWARD, data)
    tc, ts = ctw[0], ctw[1]
    rows = []
    for t in range(5):
        yr, yi = y[:128, t * 128 : (t + 1) * 128], y[128:, t * 128 : (t + 1) * 128]
        rows.append(jnp.concatenate([yr * tc + yi * ts, yi * tc - yr * ts], axis=1))
    f = times_table(mats, LANES, jnp.concatenate(rows, axis=0))
    ky2 = lane // 4
    col = lane % 4
    ky = sub + 128 * ky2
    nyquist = ky == 2048
    ky = jnp.where(ky >= 2048, ky - 4096, ky).astype(F32)
    scale = 1.0 / (float(N) * float(N))
    hats = []
    for t in range(5):
        fr, fi = f[t * 128 : (t + 1) * 128, :128], f[t * 128 : (t + 1) * 128, 128:]
        if t < 4:
            slot = t * 4 + col
            kx = slot + 32 * me
            if t == 0:
                zeroth = jnp.where(
                    me < 64, 16 + 32 * me, jnp.where(me == 64, 0, 32 * me)
                )
                kx = jnp.where(slot == 0, zeroth, kx)
            kx = jnp.where(kx >= 2048, kx - 4096, kx).astype(F32)
        else:
            kx = jnp.full((128, 128), -2048.0, F32)
        norm = kx * kx + ky * ky
        if t == 0:
            anchor = norm == 0
            norm = jnp.where(anchor, 1.0, norm)
            fr, fi = jnp.where(anchor, 0.0, fr), jnp.where(anchor, 0.0, fi)
        power[t] = fr * fr + fi * fi
        inv = scale / norm
        kr = (kx * kx - ky * ky) * inv
        ki = 2.0 * kx * ky * inv
        if t < 4:
            kn = jnp.where(nyquist, ki, 0.0)
            ki = jnp.where(nyquist, 0.0, ki)
            a = (kr * fr - kn * fi, kr * fi + kn * fr)
            c = (ki * fr, ki * fi)
        else:
            kn = jnp.where(nyquist, ki, 0.0)
            ki = jnp.where(nyquist, 0.0, ki)
            a = (kr * fr - ki * fi, kr * fi + ki * fr)
            c = (kn * fr, kn * fi)
        hats.append((a, c))
    rows = [jnp.concatenate(hats[t][ac], axis=1) for ac in range(2) for t in range(5)]
    g = times_table(mats, LANES_BACK, jnp.concatenate(rows, axis=0))
    re, im = [], []
    for i in range(10):
        gr, gi = g[i * 128 : (i + 1) * 128, :128], g[i * 128 : (i + 1) * 128, 128:]
        re.append(gr * tc - gi * ts)
        im.append(gi * tc + gr * ts)
    data = jnp.concatenate([jnp.concatenate(re, axis=1), jnp.concatenate(im, axis=1)], axis=0)
    s = table_times(mats, INVERSE, data)
    for ac in range(2):
        for t in range(4):
            at = (ac * 5 + t) * 128
            sr, si = s[:128, at : at + 128], s[128:, at : at + 128]
            if t == 0:
                extra = (ac * 5 + 4) * 128
                si = jnp.where(special, s[:128, extra : extra + 128], si)
            msg[pl.ds(ac * 8 + t, 128, stride=16), :] = sr
            msg[pl.ds(ac * 8 + 4 + t, 128, stride=16), :] = si


def row_inverse(recv, mats, rtw, vbuf, outs):
    lane = lax.broadcasted_iota(jnp.int32, (256, 128), 1)
    for ac in range(2):
        parts = [
            jnp.concatenate(
                [recv[pl.ds(ac * 8 + c * 4 + t, 128, stride=16), :] for t in range(4)], axis=1
            )
            for c in range(2)
        ]
        data = jnp.concatenate(parts, axis=0)
        v = table_times(mats, INVERSE, data)
        special = table_times(mats, BACK, data[:, :128])
        first = jnp.where(lane < 32, special, v[:, :128])
        for c in range(2):
            rows = slice(c * 128, (c + 1) * 128)
            full = jnp.concatenate([first[rows], v[rows, 128:]], axis=1)
            vbuf[c] = full.T
        for q in range(4):
            g = [None] * 17
            for k1 in range(16):
                at = pl.ds(k1 * 32 + q * 8, 8)
                vr, vi = vbuf[0, at, :], vbuf[1, at, :]
                if k1 == 0:
                    g[0], g[16] = (vr, None), (vi, None)
                else:
                    tr, ti = rtw[0, pl.ds(k1, 1), :], rtw[1, pl.ds(k1, 1), :]
                    g[k1] = (vr * tr - vi * ti, vi * tr + vr * ti)
            out = irfft(g)
            for x1 in range(32):
                outs[ac][pl.ds(q * 8, 8), pl.ds(x1 * 128, 128)] = out[x1]


STRIDE = 37


def peer(me, i):
    return lax.rem(me + i * STRIDE, DEVICES)


def send_all(me, msg, recv, send, arrive, rows):
    def step(i, _):
        to = peer(me, i)
        pltpu.make_async_remote_copy(
            src_ref=msg.at[pl.ds(pl.multiple_of(to * rows, rows), rows)],
            dst_ref=recv.at[pl.ds(pl.multiple_of(me * rows, rows), rows)],
            send_sem=send,
            recv_sem=arrive,
            device_id=to,
            device_id_type=LOGICAL,
        ).start()
        return 0

    lax.fori_loop(1, DEVICES, step, 0)
    own = pl.ds(pl.multiple_of(me * rows, rows), rows)
    recv[own, :] = msg[own, :]


def wait_all(buf, sem, rows):
    part = buf.at[pl.ds(0, (DEVICES - 1) * rows)]
    pltpu.make_async_copy(part, part, sem).wait()


def arrange_bins(me, raw, near, far):
    row = lax.broadcasted_iota(jnp.int32, (128, 128), 0)
    lane = lax.broadcasted_iota(jnp.int32, (128, 128), 1)
    rcol, rky2 = row % 32, row // 32
    lcol, lky2 = lane % 4, lane // 4
    low = me < 64
    wanted = []
    for t in range(4):
        slot = 4 * t + lcol
        own, other = slot, 32 - slot
        if t == 0:
            own = jnp.where(slot == 0, jnp.where(low, 16, 0), own)
            other = jnp.where(slot == 0, jnp.where(low, 0, 16), other)
        wanted.append((rcol == own, lky2 - rky2))
        wanted.append((rcol == other, 31 - lky2 - rky2))
    wanted.append((jnp.logical_and(lcol == 0, rcol == 0), lky2 - rky2))
    sums = [jnp.zeros((128, 128), F32) for _ in wanted]
    for g in range(8):
        pieces = [raw[:, pl.ds((4 * g + i) * 128, 128)].astype(F32) for i in range(4)]
        data = jnp.concatenate(pieces, axis=0).T.astype(BF16)
        for i, (match, shift) in enumerate(wanted):
            pick = jnp.where(jnp.logical_and(match, shift == 4 * g), 1.0, 0.0).astype(BF16)
            sums[i] = sums[i] + jnp.dot(data, pick, preferred_element_type=F32)
    flip = jnp.where(jnp.logical_and(row + lane == 128, row > 0), 1.0, 0.0).astype(BF16)
    for t in range(4):
        own, other = sums[2 * t], sums[2 * t + 1]
        if t == 0:
            own = jnp.where(jnp.logical_and(lcol == 0, me == 64), float(NBINS), own)
        near[t] = own
        turned = jnp.dot(flip, other.astype(BF16), preferred_element_type=F32)
        first = jnp.concatenate([other[:1, 124:], other[:1, :124]], axis=1)
        far[t] = jnp.where(row == 0, first, turned)
    near[4] = sums[8]


def bin_power(near, far, power, acc, spec):
    def group(g, _):
        sums = [jnp.zeros((8, 128), F32) for _ in range(8)]
        for i in range(9):
            t = i % 5 if i < 5 else i - 5
            which = 0 if i < 5 else 1
            for r in range(16):
                at = pl.ds(r * 8, 8)
                b = (far if which else near)[t, at, :] - (g * 8).astype(F32)
                p = power[t, at, :]
                for k in range(8):
                    sums[k] = sums[k] + jnp.where(b == float(k), p, 0.0)
        rows = [jnp.sum(v, axis=0, keepdims=True) for v in sums]
        acc[pl.ds(pl.multiple_of(g * 8, 8), 8), :] = jnp.concatenate(rows, axis=0)
        return 0

    lax.fori_loop(0, 8, group, 0)
    acc[pl.ds(64, 64), :] = jnp.zeros((64, 128), F32)
    row = jnp.sum(acc[...].T, axis=0, keepdims=True)
    spec[0] = row * (NBINS / float(N) ** 4)


def reduce_planes(idle, mine, res, yf, zf, yrelay, ydirect, yfinal, zrecv, zsum, ssem, rsem):
    y, zh = lax.axis_index("y"), lax.axis_index("zh")
    base = my_index() - y * 2 - zh
    up, down, across = lax.rem(y + 1, 4), lax.rem(y + 3, 4), lax.rem(y + 2, 4)
    dev_up, dev_down = base + up * 2 + zh, base + down * 2 + zh
    dev_z = base + y * 2 + (1 - zh)
    count = [0]
    sends = []

    def send(src, dst, to):
        i = count[0]
        count[0] += 1
        copy = pltpu.make_async_remote_copy(
            src_ref=src,
            dst_ref=dst,
            send_sem=ssem.at[i],
            recv_sem=rsem.at[i],
            device_id=to,
            device_id_type=LOGICAL,
        )
        copy.start()
        sends.append(copy)
        return copy

    def share(t, h, q):
        return mine.at[pl.ds(pl.multiple_of((t * 2 + h) * 32 + q * 8, 8), 8)]

    znew = {}
    for q in zf:
        for i, t in enumerate((across, up, down, y)):
            znew[q, i] = send(share(t, 1 - zh, q), zrecv.at[q, i], dev_z)
    relay, direct, final = {}, {}, {}
    for q in yf:
        relay[q, 0] = send(share(across, 0, q), yrelay.at[q, 0], dev_up)
        relay[q, 1] = send(share(across, 1, q), yrelay.at[q, 1], dev_down)
        direct[q, 0] = send(share(up, 1, q), ydirect.at[q, 1], dev_up)
        direct[q, 1] = send(share(down, 0, q), ydirect.at[q, 0], dev_down)
    half = (slice(0, 2048), slice(2048, 4096))

    def y_relay_first(q):
        relay[q, 0].wait_recv()
        yrelay[q, 0] = yrelay[q, 0] + share(up, 0, q)[...]
        final[q, 0] = send(yrelay.at[q, 0], yfinal.at[q, 0], dev_up)
        relay[q, 1].wait_recv()
        yrelay[q, 1] = yrelay[q, 1] + share(down, 1, q)[...]
        final[q, 1] = send(yrelay.at[q, 1], yfinal.at[q, 1], dev_down)

    def y_finish_first(q):
        for h in range(2):
            direct[q, h].wait_recv()
            final[q, h].wait_recv()
        for h in range(2):
            yfinal[q, h] = yfinal[q, h] + ydirect[q, h] + share(y, h, q)[...]
        znew[q, 0] = send(yfinal.at[q, 1 - zh], zrecv.at[q, 0], dev_z)

    def z_last(q):
        znew[q, 0].wait_recv()
        res[pl.ds(q * 8, 8), :] = zrecv[q, 0] + yfinal[q, zh]

    def z_first(q):
        for i, t in enumerate((across, up, down, y)):
            znew[q, i].wait_recv()
            zsum[q, i] = zrecv[q, i] + share(t, zh, q)[...]
            if i == 0:
                relay[q, 0] = send(
                    zsum.at[q, 0, :, pl.ds(0, 2048)], yrelay.at[q, 0, :, pl.ds(0, 2048)], dev_up
                )
                relay[q, 1] = send(
                    zsum.at[q, 0, :, pl.ds(2048, 2048)], yrelay.at[q, 1, :, pl.ds(0, 2048)], dev_down
                )
            if i == 1:
                direct[q, 0] = send(
                    zsum.at[q, 1, :, pl.ds(2048, 2048)], ydirect.at[q, 1, :, pl.ds(0, 2048)], dev_up
                )
            if i == 2:
                direct[q, 1] = send(
                    zsum.at[q, 2, :, pl.ds(0, 2048)], ydirect.at[q, 0, :, pl.ds(0, 2048)], dev_down
                )

    def y_relay_last(q):
        relay[q, 0].wait_recv()
        yrelay[q, 0, :, :2048] = yrelay[q, 0, :, :2048] + zsum[q, 1, :, half[0]]
        final[q, 0] = send(
            yrelay.at[q, 0, :, pl.ds(0, 2048)], yfinal.at[q, 0, :, pl.ds(0, 2048)], dev_up
        )
        relay[q, 1].wait_recv()
        yrelay[q, 1, :, :2048] = yrelay[q, 1, :, :2048] + zsum[q, 2, :, half[1]]
        final[q, 1] = send(
            yrelay.at[q, 1, :, pl.ds(0, 2048)], yfinal.at[q, 1, :, pl.ds(0, 2048)], dev_down
        )

    def y_last(q):
        for h in range(2):
            direct[q, h].wait_recv()
            final[q, h].wait_recv()
        for h in range(2):
            res[pl.ds(q * 8, 8), half[h]] = (
                zsum[q, 3, :, half[h]] + yfinal[q, h, :, :2048] + ydirect[q, h, :, :2048]
            )

    y_relay_first(yf[0])
    idle()
    y_relay_first(yf[1])
    y_finish_first(yf[0])
    z_first(zf[0])
    y_relay_last(zf[0])
    y_finish_first(yf[1])
    z_first(zf[1])
    y_relay_last(zf[1])
    y_last(zf[0])
    z_last(yf[0])
    z_last(yf[1])
    y_last(zf[1])
    return sends


def kernel(
    density, weight, bins_in, mats_in, out_real, out_imag, out_spec,
    recvc, specs, ctw, rtw, mine, res, mats, yrelay, ydirect, yfinal, zrecv, zsum,
    ubuf, msgb, recvb, msgc, power, acc, spec, raw, near, far, farin, extra,
    lsem, msem, bsem, fsem, ssem, rsem, asem,
):
    me = my_index()
    barrier = pltpu.get_barrier_semaphore()
    loads = []
    for i in range(8):
        copy = pltpu.make_async_copy(
            density.at[0, pl.ds(i * 32, 32)], mine.at[pl.ds(i * 32, 32)], lsem.at[i]
        )
        copy.start()
        loads.append(copy)
    mload = pltpu.make_async_copy(mats_in, mats, msem)
    mload.start()
    bload = pltpu.make_async_copy(bins_in, raw, bsem)
    bload.start()

    def greet(i, _):
        pl.semaphore_signal(
            barrier, inc=1, device_id=lax.rem(me + i, DEVICES), device_id_type=LOGICAL
        )
        return 0

    lax.fori_loop(1, DEVICES, greet, 0)
    w = weight[0]
    for i in range(8):
        loads[i].wait()
        rows = pl.ds(i * 32, 32)
        mine[rows, :] = mine[rows, :] * w
    pl.semaphore_wait(barrier, DEVICES - 1)

    def idle():
        mload.wait()
        read_twiddles(mats, ctw, rtw)
        bload.wait()
        arrange_bins(me, raw, near, far)

    sends = reduce_planes(
        idle, mine, res, (0, 1), (2, 3), yrelay, ydirect, yfinal, zrecv, zsum, ssem, rsem
    )
    row_forward(res, mats, rtw, ubuf, msgb)
    send_all(me, msgb, recvb, asem.at[0], asem.at[1], 8)
    mirror = pltpu.make_async_remote_copy(
        src_ref=far,
        dst_ref=farin,
        send_sem=fsem.at[0],
        recv_sem=fsem.at[1],
        device_id=DEVICES - 1 - me,
        device_id_type=LOGICAL,
    )
    mirror.start()
    zeroth = pltpu.make_async_remote_copy(
        src_ref=far.at[0],
        dst_ref=extra,
        send_sem=fsem.at[2],
        recv_sem=fsem.at[3],
        device_id=jnp.where(me == 0, 64, DEVICES - me),
        device_id_type=LOGICAL,
    )

    @pl.when(me < 64)
    def _():
        zeroth.start()

    wait_all(recvb, asem.at[1], 8)
    column_part(me, recvb, mats, ctw, power, msgc)
    send_all(me, msgc, recvc, asem.at[2], asem.at[3], 16)
    mirror.wait_recv()

    @pl.when(me >= 64)
    def _():
        zeroth.wait_recv()
        lane = lax.broadcasted_iota(jnp.int32, (128, 128), 1)
        farin[0] = jnp.where(lane % 4 == 0, extra[...], farin[0])

    bin_power(near, farin, power, acc, spec)

    def share_spec(i, _):
        to = peer(me, i)
        pltpu.make_async_remote_copy(
            src_ref=spec.at[0],
            dst_ref=specs.at[me],
            send_sem=asem.at[4],
            recv_sem=asem.at[5],
            device_id=to,
            device_id_type=LOGICAL,
        ).start()
        return 0

    lax.fori_loop(1, DEVICES, share_spec, 0)
    specs[me] = spec[0]
    wait_all(recvc, asem.at[3], 16)
    row_inverse(recvc, mats, rtw, ubuf, (out_real, out_imag))
    wait_all(specs, asem.at[5], 1)
    total = specs[0]
    for i in range(1, DEVICES):
        total = total + specs[i]
    out_spec[...] = total[:, :NBINS]
    wait_all(msgb, asem.at[0], 8)
    wait_all(msgc, asem.at[2], 16)
    wait_all(specs, asem.at[4], 1)
    for copy in sends:
        copy.wait_send()
    mirror.wait_send()

    @pl.when(me < 64)
    def _():
        zeroth.wait_send()


def finish(*refs):
    sems = refs[6]
    copies = [pltpu.make_async_copy(refs[i], refs[3 + i], sems.at[i]) for i in range(3)]
    for copy in copies:
        copy.start()
    for copy in copies:
        copy.wait()


def on_device(mats, density, lens_weight, spectrum_bin):
    vmem = pl.BlockSpec(memory_space=pltpu.VMEM)
    hbm = pl.BlockSpec(memory_space=pltpu.HBM)
    smem = pl.BlockSpec(memory_space=pltpu.SMEM)
    dma = pltpu.SemaphoreType.DMA
    share = (8, 4096)
    params = partial(pltpu.CompilerParams, vmem_limit_bytes=55050240)
    shapes = (
        jax.ShapeDtypeStruct((32, N), F32),
        jax.ShapeDtypeStruct((32, N), F32),
        jax.ShapeDtypeStruct((1, NBINS), F32),
    )
    results = pl.pallas_call(
        kernel,
        name="shear",
        out_shape=shapes,
        in_specs=[hbm, smem, hbm, hbm],
        out_specs=(vmem, vmem, vmem),
        scratch_shapes=[
            pltpu.VMEM((DEVICES * 16, 128), F32),
            pltpu.VMEM((DEVICES, 1, 128), F32),
            pltpu.VMEM((2, 128, 128), F32),
            pltpu.VMEM((2, 16, 128), F32),
            pltpu.VMEM((256, N), F32),
            pltpu.VMEM((32, N), F32),
            pltpu.VMEM((7, 2, 256, 256), BF16),
            pltpu.VMEM((4, 2) + share, F32),
            pltpu.VMEM((4, 2) + share, F32),
            pltpu.VMEM((4, 2) + share, F32),
            pltpu.VMEM((4, 4) + share, F32),
            pltpu.VMEM((4, 4) + share, F32),
            pltpu.VMEM((2, 512, 128), F32),
            pltpu.VMEM((DEVICES * 8, 128), F32),
            pltpu.VMEM((DEVICES * 8, 128), F32),
            pltpu.VMEM((DEVICES * 16, 128), F32),
            pltpu.VMEM((5, 128, 128), F32),
            pltpu.VMEM((128, 128), F32),
            pltpu.VMEM((1, 1, 128), F32),
            pltpu.VMEM((32, N), jnp.int32),
            pltpu.VMEM((5, 128, 128), F32),
            pltpu.VMEM((4, 128, 128), F32),
            pltpu.VMEM((4, 128, 128), F32),
            pltpu.VMEM((128, 128), F32),
            dma((8,)),
            dma,
            dma,
            dma((4,)),
            dma((40,)),
            dma((40,)),
            dma((6,)),
        ],
        compiler_params=params(collective_id=0, has_side_effects=True),
    )(density, lens_weight, spectrum_bin.T, mats)
    real, imag, spectrum = pl.pallas_call(
        finish,
        name="finish",
        out_shape=shapes,
        in_specs=[vmem, vmem, vmem],
        out_specs=(hbm, hbm, hbm),
        scratch_shapes=[dma((3,))],
        compiler_params=params(),
    )(*results)
    return real, imag, spectrum.reshape(NBINS)


def solution(mesh):
    finer = Mesh(mesh.devices.reshape(4, 2, 2, 4, 2), AXES)
    tables = jnp.asarray(make_tables())
    step = jax.shard_map(
        on_device,
        mesh=finer,
        in_specs=(P(), P(PLANES, ROWS, None), P(PLANES), P(None, AXES)),
        out_specs=(P(AXES, None), P(AXES, None), P()),
        check_vma=False,
    )

    def whole(density, lens_weight, spectrum_bin):
        return step(tables, density, lens_weight, spectrum_bin)

    return whole
```

```python
from functools import partial
import math

import jax
import jax.numpy as jnp
import ml_dtypes
import numpy as np
from jax import lax
from jax.experimental import pallas as pl
from jax.experimental.pallas import tpu as pltpu
from jax.sharding import Mesh
from jax.sharding import PartitionSpec as P

N = 4096
NBINS = 64
DEVICES = 128
AXES = ("x", "zl", "core", "y", "zh")
ROWS = ("x", "zl", "core")
PLANES = ("y", "zh")
LOGICAL = pl.DeviceIdType.LOGICAL
F32 = jnp.float32
BF16 = jnp.bfloat16


def halves(table):
    high = table.astype(np.float32).astype(ml_dtypes.bfloat16)
    low = (table - high.astype(np.float64)).astype(np.float32).astype(ml_dtypes.bfloat16)
    return np.stack([high, low])


def make_tables():
    turn = 2.0 * math.pi
    i128 = np.arange(128)
    angle = turn * ((i128[:, None] * i128[None, :]) % 128) / 128
    cos, sin = np.cos(angle), np.sin(angle)
    forward = np.block([[cos, sin], [-sin, cos]])
    inverse = np.block([[cos, -sin], [sin, cos]])
    first = np.zeros((256, 256))
    back = np.zeros((256, 256))
    for d in range(128):
        if d < 64:
            phase = turn * (((16 + 32 * d) * i128) % 4096) / 4096
            first[d, 128:] = np.cos(phase)
            first[128 + d, 128:] = -np.sin(phase)
            weight = 2.0
        elif d == 64:
            first[d, :128] = 1.0
            first[128 + d, :128] = (-1.0) ** i128
            weight = 1.0
        else:
            phase = turn * ((d * i128) % 128) / 128
            first[d, :128] = np.cos(phase)
            first[128 + d, :128] = -np.sin(phase)
            weight = 2.0
        back[:, d] = weight * first[d]
        back[:, 128 + d] = weight * first[128 + d]
    small = np.zeros((4, 32, 32, 4), np.complex128)
    i32 = np.arange(32)
    kernel = np.exp(-1j * turn * ((i32[:, None] * i32[None, :]) % 32) / 32)
    for c in range(4):
        small[c, :, :, c] = kernel
    small = small.reshape(128, 128)
    lanes = np.block([[small.real, small.imag], [-small.imag, small.real]])
    wide = np.conj(small).T
    lanes_back = np.block([[wide.real, wide.imag], [-wide.imag, wide.real]])
    mats = np.stack([halves(t) for t in (forward, inverse, first, back, lanes, lanes_back)])
    y2 = np.tile(i32, 4)
    phase = turn * (i128[:, None] * y2[None, :]) / 4096
    column_twiddle = np.stack([np.cos(phase), np.sin(phase)]).astype(np.float32)
    phase = turn * (np.arange(16)[:, None] * i128[None, :]) / 4096
    row_twiddle = np.stack([np.cos(phase), np.sin(phase)]).astype(np.float32)
    extra = np.zeros((1, 2, 256, 256), ml_dtypes.bfloat16)
    for c in range(2):
        for j, (up, left) in enumerate(((0, 0), (0, 128), (128, 0))):
            part = column_twiddle[c].astype(ml_dtypes.bfloat16)
            column_twiddle[c] -= part.astype(np.float32)
            extra[0, c, up : up + 128, left : left + 128] = part
            part = row_twiddle[c].astype(ml_dtypes.bfloat16)
            row_twiddle[c] -= part.astype(np.float32)
            extra[0, c, 128 + 16 * j : 144 + 16 * j, 128:] = part
    return np.concatenate([mats, extra])


FORWARD, INVERSE, FIRST, BACK, LANES, LANES_BACK, TWIDDLES = range(7)


def rfft(values):
    n = len(values)
    if n == 2:
        return [(values[0] + values[1], None), (values[0] - values[1], None)]
    even, odd = rfft(values[0::2]), rfft(values[1::2])
    out = [None] * (n // 2 + 1)
    out[0] = (even[0][0] + odd[0][0], None)
    out[n // 2] = (even[0][0] - odd[0][0], None)
    for k in range(1, n // 4):
        c, s = math.cos(2 * math.pi * k / n), math.sin(2 * math.pi * k / n)
        er, ei = even[k]
        orr, oi = odd[k]
        if 8 * k == n:
            pr, pi = (orr + oi) * c, (oi - orr) * c
        else:
            pr, pi = orr * c + oi * s, oi * c - orr * s
        out[k] = (er + pr, ei + pi)
        out[n // 2 - k] = (er - pr, pi - ei)
    out[n // 4] = (even[n // 4][0], -odd[n // 4][0])
    return out


def irfft(g):
    n = 2 * (len(g) - 1)
    if n == 2:
        return [g[0][0] + g[1][0], g[0][0] - g[1][0]]
    even, odd = [None] * (n // 4 + 1), [None] * (n // 4 + 1)
    even[0] = (g[0][0] + g[n // 2][0], None)
    odd[0] = (g[0][0] - g[n // 2][0], None)
    for k in range(1, n // 4):
        c, s = math.cos(2 * math.pi * k / n), math.sin(2 * math.pi * k / n)
        ar, ai = g[k]
        br, bi = g[n // 2 - k]
        even[k] = (ar + br, ai - bi)
        dr, di = ar - br, ai + bi
        odd[k] = (dr * c - di * s, dr * s + di * c)
    mr, mi = g[n // 4]
    even[n // 4] = (mr + mr, None)
    odd[n // 4] = (-(mi + mi), None)
    a, b = irfft(even), irfft(odd)
    out = [None] * n
    out[0::2], out[1::2] = a, b
    return out


def split(value):
    high = value.astype(BF16)
    return high, (value - high.astype(F32)).astype(BF16)


def table_times(mats, which, data):
    high, low = split(data)
    dot = partial(jnp.dot, preferred_element_type=F32)
    return dot(mats[which, 0], high) + dot(mats[which, 0], low) + dot(mats[which, 1], high)


def times_table(mats, which, data):
    high, low = split(data)
    dot = partial(jnp.dot, preferred_element_type=F32)
    return dot(high, mats[which, 0]) + dot(low, mats[which, 0]) + dot(high, mats[which, 1])


def read_twiddles(mats, ctw, rtw):
    for c in range(2):
        parts = [
            mats[TWIDDLES, c, pl.ds(up, 128), pl.ds(left, 128)].astype(F32)
            for up, left in ((0, 0), (0, 128), (128, 0))
        ]
        ctw[c] = parts[0] + parts[1] + parts[2]
        parts = [
            mats[TWIDDLES, c, pl.ds(128 + 16 * j, 16), pl.ds(128, 128)].astype(F32)
            for j in range(3)
        ]
        rtw[c] = parts[0] + parts[1] + parts[2]


def my_index():
    x, zl, core, y, zh = (lax.axis_index(a) for a in AXES)
    return ((x * 2 + zl) * 2 + core) * 8 + y * 2 + zh


def row_forward(b, w, mine, mats, rtw, ubuf, spread):
    for q in range(4):
        rows = pl.ds(b * 32 + q * 8, 8)
        out = rfft([mine[rows, pl.ds(x1 * 128, 128)] * w for x1 in range(32)])
        for k1 in range(16):
            at = pl.ds(k1 * 32 + q * 8, 8)
            if k1 == 0:
                ubuf[0, at, :], ubuf[1, at, :] = out[0][0], out[16][0]
            else:
                tr, ti = rtw[0, pl.ds(k1, 1), :], rtw[1, pl.ds(k1, 1), :]
                ur, ui = out[k1]
                ubuf[0, at, :] = ur * tr + ui * ti
                ubuf[1, at, :] = ui * tr - ur * ti
    data = jnp.concatenate([ubuf[0].T, ubuf[1].T], axis=0)
    out = table_times(mats, FORWARD, data)
    special = table_times(mats, FIRST, data[:, :128])
    lane = lax.broadcasted_iota(jnp.int32, (256, 128), 1)
    for t in range(4):
        piece = out[:, t * 128 : (t + 1) * 128]
        if t == 0:
            piece = jnp.where(lane < 32, special, piece)
        for c in range(2):
            for r in range(16):
                at = c * 128 + r * 8
                spread[pl.ds(b * 1024 + r * 8 + c * 4 + t, 8, stride=128), :] = piece[at : at + 8]


def column_part(me, recv, mats, ctw, power, msg, send):
    lane = lax.broadcasted_iota(jnp.int32, (128, 128), 1)
    sub = lax.broadcasted_iota(jnp.int32, (128, 128), 0)
    special = jnp.logical_and(lane < 32, me == 64)
    re = [recv[pl.ds(t, 128, stride=8), :] for t in range(4)]
    im = [recv[pl.ds(4 + t, 128, stride=8), :] for t in range(4)]
    zero = jnp.zeros((128, 128), F32)
    re.append(jnp.where(special, im[0], zero))
    im[0] = jnp.where(special, zero, im[0])
    im.append(zero)
    data = jnp.concatenate([jnp.concatenate(re, axis=1), jnp.concatenate(im, axis=1)], axis=0)
    y = table_times(mats, FORWARD, data)
    tc, ts = ctw[0], ctw[1]
    rows = []
    for t in range(5):
        yr, yi = y[:128, t * 128 : (t + 1) * 128], y[128:, t * 128 : (t + 1) * 128]
        rows.append(jnp.concatenate([yr * tc + yi * ts, yi * tc - yr * ts], axis=1))
    f = times_table(mats, LANES, jnp.concatenate(rows, axis=0))
    ky2 = lane // 4
    col = lane % 4
    ky = sub + 128 * ky2
    nyquist = ky == 2048
    ky = jnp.where(ky >= 2048, ky - 4096, ky).astype(F32)
    scale = 1.0 / (float(N) * float(N))
    hats = []
    for t in range(5):
        fr, fi = f[t * 128 : (t + 1) * 128, :128], f[t * 128 : (t + 1) * 128, 128:]
        if t < 4:
            slot = t * 4 + col
            kx = slot + 32 * me
            if t == 0:
                zeroth = jnp.where(
                    me < 64, 16 + 32 * me, jnp.where(me == 64, 0, 32 * me)
                )
                kx = jnp.where(slot == 0, zeroth, kx)
            kx = jnp.where(kx >= 2048, kx - 4096, kx).astype(F32)
        else:
            kx = jnp.full((128, 128), -2048.0, F32)
        norm = kx * kx + ky * ky
        if t == 0:
            anchor = norm == 0
            norm = jnp.where(anchor, 1.0, norm)
            fr, fi = jnp.where(anchor, 0.0, fr), jnp.where(anchor, 0.0, fi)
        power[t] = fr * fr + fi * fi
        inv = scale / norm
        kr = (kx * kx - ky * ky) * inv
        ki = 2.0 * kx * ky * inv
        if t < 4:
            kn = jnp.where(nyquist, ki, 0.0)
            ki = jnp.where(nyquist, 0.0, ki)
            a = (kr * fr - kn * fi, kr * fi + kn * fr)
            c = (ki * fr, ki * fi)
        else:
            kn = jnp.where(nyquist, ki, 0.0)
            ki = jnp.where(nyquist, 0.0, ki)
            a = (kr * fr - ki * fi, kr * fi + ki * fr)
            c = (kn * fr, kn * fi)
        hats.append((a, c))
    for ac in range(2):
        rows = [jnp.concatenate(hats[t][ac], axis=1) for t in range(5)]
        g = times_table(mats, LANES_BACK, jnp.concatenate(rows, axis=0))
        re, im = [], []
        for t in range(5):
            gr, gi = g[t * 128 : (t + 1) * 128, :128], g[t * 128 : (t + 1) * 128, 128:]
            re.append(gr * tc - gi * ts)
            im.append(gi * tc + gr * ts)
        data = jnp.concatenate([jnp.concatenate(re, axis=1), jnp.concatenate(im, axis=1)], axis=0)
        s = table_times(mats, INVERSE, data)
        for t in range(4):
            sr, si = s[:128, t * 128 : (t + 1) * 128], s[128:, t * 128 : (t + 1) * 128]
            if t == 0:
                si = jnp.where(special, s[:128, 512:], si)
            msg[pl.ds(ac * 1024 + t, 128, stride=8), :] = sr
            msg[pl.ds(ac * 1024 + 4 + t, 128, stride=8), :] = si
        send(ac)


def row_inverse(ac, recv, mats, rtw, vbuf, out_ref):
    lane = lax.broadcasted_iota(jnp.int32, (256, 128), 1)
    parts = [
        jnp.concatenate(
            [recv[pl.ds(ac * 1024 + c * 4 + t, 128, stride=8), :] for t in range(4)], axis=1
        )
        for c in range(2)
    ]
    data = jnp.concatenate(parts, axis=0)
    v = table_times(mats, INVERSE, data)
    special = table_times(mats, BACK, data[:, :128])
    first = jnp.where(lane < 32, special, v[:, :128])
    for c in range(2):
        rows = slice(c * 128, (c + 1) * 128)
        full = jnp.concatenate([first[rows], v[rows, 128:]], axis=1)
        vbuf[c] = full.T
    for q in range(4):
        g = [None] * 17
        for k1 in range(16):
            at = pl.ds(k1 * 32 + q * 8, 8)
            vr, vi = vbuf[0, at, :], vbuf[1, at, :]
            if k1 == 0:
                g[0], g[16] = (vr, None), (vi, None)
            else:
                tr, ti = rtw[0, pl.ds(k1, 1), :], rtw[1, pl.ds(k1, 1), :]
                g[k1] = (vr * tr - vi * ti, vi * tr + vr * ti)
        out = irfft(g)
        for x1 in range(32):
            out_ref[pl.ds(q * 8, 8), pl.ds(x1 * 128, 128)] = out[x1]


STRIDE = 107


def peer(me, i):
    return lax.rem(me + i * STRIDE, DEVICES)


def send_all(me, half, msg, recv, send, arrive):
    def block(d):
        return pl.ds(pl.multiple_of((half * DEVICES + d) * 8, 8), 8)

    def step(i, _):
        to = peer(me, i)
        pltpu.make_async_remote_copy(
            src_ref=msg.at[block(to)],
            dst_ref=recv.at[block(me)],
            send_sem=send,
            recv_sem=arrive,
            device_id=to,
            device_id_type=LOGICAL,
        ).start()
        return 0

    lax.fori_loop(1, DEVICES, step, 0)
    recv[block(me), :] = msg[block(me), :]


def wait_all(buf, sem, rows, count=DEVICES - 1):
    part = buf.at[pl.ds(0, count * rows)]
    pltpu.make_async_copy(part, part, sem).wait()


def arrange_bins(me, raw, near, far):
    row = lax.broadcasted_iota(jnp.int32, (128, 128), 0)
    lane = lax.broadcasted_iota(jnp.int32, (128, 128), 1)
    rcol, rky2 = row % 32, row // 32
    lcol, lky2 = lane % 4, lane // 4
    low = me < 64
    wanted = []
    for t in range(4):
        slot = 4 * t + lcol
        own, other = slot, 32 - slot
        if t == 0:
            own = jnp.where(slot == 0, jnp.where(low, 16, 0), own)
            other = jnp.where(slot == 0, jnp.where(low, 0, 16), other)
        wanted.append((rcol == own, lky2 - rky2))
        wanted.append((rcol == other, 31 - lky2 - rky2))
    wanted.append((jnp.logical_and(lcol == 0, rcol == 0), lky2 - rky2))
    sums = [jnp.zeros((128, 128), F32) for _ in wanted]
    for g in range(8):
        pieces = [raw[:, pl.ds((4 * g + i) * 128, 128)].astype(F32) for i in range(4)]
        data = jnp.concatenate(pieces, axis=0).T.astype(BF16)
        for i, (match, shift) in enumerate(wanted):
            pick = jnp.where(jnp.logical_and(match, shift == 4 * g), 1.0, 0.0).astype(BF16)
            sums[i] = sums[i] + jnp.dot(data, pick, preferred_element_type=F32)
    flip = jnp.where(jnp.logical_and(row + lane == 128, row > 0), 1.0, 0.0).astype(BF16)
    for t in range(4):
        own, other = sums[2 * t], sums[2 * t + 1]
        if t == 0:
            own = jnp.where(jnp.logical_and(lcol == 0, me == 64), float(NBINS), own)
        near[t] = own
        turned = jnp.dot(flip, other.astype(BF16), preferred_element_type=F32)
        first = jnp.concatenate([other[:1, 124:], other[:1, :124]], axis=1)
        far[t] = jnp.where(row == 0, first, turned)
    near[4] = sums[8]


def bin_power(near, far, power, acc, spec):
    def group(g, _):
        sums = [jnp.zeros((8, 128), F32) for _ in range(8)]
        for i in range(9):
            t = i % 5 if i < 5 else i - 5
            which = 0 if i < 5 else 1
            for r in range(16):
                at = pl.ds(r * 8, 8)
                b = (far if which else near)[t, at, :] - (g * 8).astype(F32)
                p = power[t, at, :]
                for k in range(8):
                    sums[k] = sums[k] + jnp.where(b == float(k), p, 0.0)
        rows = [jnp.sum(v, axis=0, keepdims=True) for v in sums]
        acc[pl.ds(pl.multiple_of(g * 8, 8), 8), :] = jnp.concatenate(rows, axis=0)
        return 0

    lax.fori_loop(0, 8, group, 0)
    acc[pl.ds(64, 64), :] = jnp.zeros((64, 128), F32)
    row = jnp.sum(acc[...].T, axis=0, keepdims=True)
    spec[0] = row * (NBINS / float(N) ** 4)


class Reduction:
    def __init__(self, spread, total, yrelay, ydirect, yfinal, zrecv, zsum, ssem, rsem):
        self.spread, self.total, self.zrecv, self.zsum = spread, total, zrecv, zsum
        self.yrelay, self.ydirect, self.yfinal = yrelay, ydirect, yfinal
        self.ssem, self.rsem, self.sends = ssem, rsem, []
        y, zh = lax.axis_index("y"), lax.axis_index("zh")
        base = my_index() - y * 2 - zh
        up, down, across = lax.rem(y + 1, 4), lax.rem(y + 3, 4), lax.rem(y + 2, 4)
        self.y, self.zh, self.turn = y, zh, (across, up, down, y)
        self.dev_up, self.dev_down = base + up * 2 + zh, base + down * 2 + zh
        self.dev_z = base + y * 2 + (1 - zh)
        self.moves = {}

    def send(self, key, src, dst, to):
        i = len(self.sends)
        copy = pltpu.make_async_remote_copy(
            src_ref=src,
            dst_ref=dst,
            send_sem=self.ssem.at[i],
            recv_sem=self.rsem.at[i],
            device_id=to,
            device_id_type=LOGICAL,
        )
        copy.start()
        self.sends.append(copy)
        self.moves[key] = copy

    def arrived(self, *keys):
        for key in keys:
            self.moves[key].wait_recv()

    def share(self, t, h, b):
        return self.spread.at[pl.ds(pl.multiple_of(b * 1024 + (t * 2 + h) * 128, 128), 128)]


    def y_start(self, b):
        across, up, down, _ = self.turn
        self.send(("relay", b, 0), self.share(across, 0, b), self.yrelay.at[b, 0], self.dev_up)
        self.send(("relay", b, 1), self.share(across, 1, b), self.yrelay.at[b, 1], self.dev_down)
        self.send(("direct", b, 0), self.share(up, 1, b), self.ydirect.at[b, 1], self.dev_up)
        self.send(("direct", b, 1), self.share(down, 0, b), self.ydirect.at[b, 0], self.dev_down)

    def y_relay(self, b):
        for h, t, to in ((0, self.turn[1], self.dev_up), (1, self.turn[2], self.dev_down)):
            self.arrived(("relay", b, h))
            self.yrelay[b, h] = self.yrelay[b, h] + self.share(t, h, b)[...]
            self.send(("final", b, h), self.yrelay.at[b, h], self.yfinal.at[b, h], to)

    def y_finish(self, b):
        self.arrived(("direct", b, 0), ("direct", b, 1), ("final", b, 0), ("final", b, 1))
        for h in range(2):
            own = self.share(self.y, h, b)[...]
            self.yfinal[b, h] = self.yfinal[b, h] + self.ydirect[b, h] + own
        self.send(("z", b, 0), self.yfinal.at[b, 1 - self.zh], self.zrecv.at[b, 0], self.dev_z)

    def z_last(self, b):
        self.arrived(("z", b, 0))
        self.total[b] = self.zrecv[b, 0] + self.yfinal[b, self.zh]


    def z_start(self, b):
        for i, t in enumerate(self.turn):
            self.send(("z", b, i), self.share(t, 1 - self.zh, b), self.zrecv.at[b, i], self.dev_z)

    def z_then_y(self, b):
        low, high = pl.ds(0, 64), pl.ds(64, 64)
        zsum = self.zsum
        for i, t in enumerate(self.turn):
            self.arrived(("z", b, i))
            zsum[b, i] = self.zrecv[b, i] + self.share(t, self.zh, b)[...]
            if i == 0:
                up, down = self.yrelay.at[b, 0, low], self.yrelay.at[b, 1, low]
                self.send(("relay", b, 0), zsum.at[b, 0, low], up, self.dev_up)
                self.send(("relay", b, 1), zsum.at[b, 0, high], down, self.dev_down)
            if i == 1:
                up = self.ydirect.at[b, 1, low]
                self.send(("direct", b, 0), zsum.at[b, 1, high], up, self.dev_up)
            if i == 2:
                down = self.ydirect.at[b, 0, low]
                self.send(("direct", b, 1), zsum.at[b, 2, low], down, self.dev_down)

    def y_relay_half(self, b):
        low = pl.ds(0, 64)
        for h, i, to in ((0, 1, self.dev_up), (1, 2, self.dev_down)):
            self.arrived(("relay", b, h))
            own = self.zsum[b, i, pl.ds(h * 64, 64)]
            self.yrelay[b, h, low] = self.yrelay[b, h, low] + own
            self.send(("final", b, h), self.yrelay.at[b, h, low], self.yfinal.at[b, h, low], to)

    def y_last(self, b):
        self.arrived(("direct", b, 0), ("direct", b, 1), ("final", b, 0), ("final", b, 1))
        low = pl.ds(0, 64)
        for h in range(2):
            rows = pl.ds(h * 64, 64)
            new = self.yfinal[b, h, low] + self.ydirect[b, h, low]
            self.total[b, rows] = self.zsum[b, 3, rows] + new


def kernel(
    density, weight, bins_in, mats_in, out_real, out_imag, out_spec,
    recvc, specs, ctw, rtw, mine, spread, total, mats, yrelay, ydirect, yfinal, zrecv, zsum,
    ubuf, recvb, msgc, power, acc, spec, raw, near, far, farin, extra,
    lsem, msem, bsem, fsem, ssem, rsem, asem,
):
    me = my_index()
    barrier = pltpu.get_barrier_semaphore()
    loads = []
    for i in range(8):
        copy = pltpu.make_async_copy(
            density.at[0, pl.ds(i * 32, 32)], mine.at[pl.ds(i * 32, 32)], lsem.at[i]
        )
        copy.start()
        loads.append(copy)
    mload = pltpu.make_async_copy(mats_in, mats, msem)
    mload.start()
    bload = pltpu.make_async_copy(bins_in, raw, bsem)
    bload.start()

    def greet(i, _):
        pl.semaphore_signal(
            barrier, inc=1, device_id=lax.rem(me + i, DEVICES), device_id_type=LOGICAL
        )
        return 0

    lax.fori_loop(1, DEVICES, greet, 0)
    w = weight[0]
    mload.wait()
    read_twiddles(mats, ctw, rtw)
    row, plane = me // 8, lax.rem(me, 8)
    red = Reduction(spread, total, yrelay, ydirect, yfinal, zrecv, zsum, ssem, rsem)

    def transform(b):
        loads[b].wait()
        row_forward(b, w, mine, mats, rtw, ubuf, spread)

    def to_columns(b):
        at = pl.ds(pl.multiple_of((row * 8 + b) * 8, 8), 8)

        def step(i, _):
            to = lax.rem(row + i * 5, 16)
            pltpu.make_async_remote_copy(
                src_ref=total.at[b, pl.ds(pl.multiple_of(to * 8, 8), 8)],
                dst_ref=recvb.at[at],
                send_sem=asem.at[0],
                recv_sem=asem.at[1],
                device_id=to * 8 + plane,
                device_id_type=LOGICAL,
            ).start()
            return 0

        lax.fori_loop(1, 16, step, 0)
        recvb[at, :] = total[b, pl.ds(pl.multiple_of(row * 8, 8), 8), :]

    transform(5)
    pl.semaphore_wait(barrier, DEVICES - 1)
    red.z_start(5)
    transform(0)
    red.y_start(0)
    transform(6)
    red.z_start(6)
    transform(1)
    red.y_start(1)
    red.y_relay(0)
    transform(7)
    red.z_start(7)
    transform(2)
    red.y_start(2)
    red.y_relay(1)
    transform(3)
    transform(4)
    red.z_then_y(5)
    red.y_start(3)
    red.y_relay(2)
    red.y_finish(0)
    red.y_relay_half(5)
    bload.wait()
    arrange_bins(me, raw, near, far)
    red.y_start(4)
    red.y_relay(3)
    red.y_finish(1)
    red.z_then_y(6)
    red.y_relay(4)
    red.y_relay_half(6)
    red.y_finish(2)
    red.y_last(5)
    to_columns(5)
    red.z_last(0)
    to_columns(0)
    red.y_finish(3)
    red.z_then_y(7)
    red.z_last(1)
    to_columns(1)
    red.y_relay_half(7)
    red.y_finish(4)
    red.y_last(6)
    to_columns(6)
    red.z_last(2)
    to_columns(2)
    red.z_last(3)
    to_columns(3)
    red.y_last(7)
    to_columns(7)
    red.z_last(4)
    to_columns(4)
    mirror = pltpu.make_async_remote_copy(
        src_ref=far,
        dst_ref=farin,
        send_sem=fsem.at[0],
        recv_sem=fsem.at[1],
        device_id=DEVICES - 1 - me,
        device_id_type=LOGICAL,
    )
    mirror.start()
    zeroth = pltpu.make_async_remote_copy(
        src_ref=far.at[0],
        dst_ref=extra,
        send_sem=fsem.at[2],
        recv_sem=fsem.at[3],
        device_id=jnp.where(me == 0, 64, DEVICES - me),
        device_id_type=LOGICAL,
    )

    @pl.when(me < 64)
    def _():
        zeroth.start()

    wait_all(recvb, asem.at[1], 8, 120)

    def to_rows(ac):
        send_all(me, ac, msgc, recvc, asem.at[2 + ac], asem.at[6 + ac])

    column_part(me, recvb, mats, ctw, power, msgc, to_rows)
    mirror.wait_recv()

    @pl.when(me >= 64)
    def _():
        zeroth.wait_recv()
        lane = lax.broadcasted_iota(jnp.int32, (128, 128), 1)
        farin[0] = jnp.where(lane % 4 == 0, extra[...], farin[0])

    bin_power(near, farin, power, acc, spec)

    def share_spec(i, _):
        to = peer(me, i)
        pltpu.make_async_remote_copy(
            src_ref=spec.at[0],
            dst_ref=specs.at[me],
            send_sem=asem.at[4],
            recv_sem=asem.at[5],
            device_id=to,
            device_id_type=LOGICAL,
        ).start()
        return 0

    lax.fori_loop(1, DEVICES, share_spec, 0)
    specs[me] = spec[0]
    wait_all(recvc, asem.at[6], 8)
    row_inverse(0, recvc, mats, rtw, ubuf, out_real)
    wait_all(recvc, asem.at[7], 8)
    row_inverse(1, recvc, mats, rtw, ubuf, out_imag)
    wait_all(specs, asem.at[5], 1)
    power_sum = specs[0]
    for i in range(1, DEVICES):
        power_sum = power_sum + specs[i]
    out_spec[...] = power_sum[:, :NBINS]
    wait_all(recvb, asem.at[0], 8, 120)
    wait_all(msgc, asem.at[2], 8)
    wait_all(msgc, asem.at[3], 8)
    wait_all(specs, asem.at[4], 1)
    for copy in red.sends:
        copy.wait_send()
    mirror.wait_send()

    @pl.when(me < 64)
    def _():
        zeroth.wait_send()


def finish(*refs):
    sems = refs[6]
    copies = [pltpu.make_async_copy(refs[i], refs[3 + i], sems.at[i]) for i in range(3)]
    for copy in copies:
        copy.start()
    for copy in copies:
        copy.wait()


def on_device(mats, density, lens_weight, spectrum_bin):
    vmem = pl.BlockSpec(memory_space=pltpu.VMEM)
    hbm = pl.BlockSpec(memory_space=pltpu.HBM)
    smem = pl.BlockSpec(memory_space=pltpu.SMEM)
    dma = pltpu.SemaphoreType.DMA
    share = (128, 128)
    params = partial(pltpu.CompilerParams, vmem_limit_bytes=55050240)
    shapes = (
        jax.ShapeDtypeStruct((32, N), F32),
        jax.ShapeDtypeStruct((32, N), F32),
        jax.ShapeDtypeStruct((1, NBINS), F32),
    )
    results = pl.pallas_call(
        kernel,
        name="shear",
        out_shape=shapes,
        in_specs=[hbm, smem, hbm, hbm],
        out_specs=(vmem, vmem, vmem),
        scratch_shapes=[
            pltpu.VMEM((DEVICES * 16, 128), F32),
            pltpu.VMEM((DEVICES, 1, 128), F32),
            pltpu.VMEM((2, 128, 128), F32),
            pltpu.VMEM((2, 16, 128), F32),
            pltpu.VMEM((256, N), F32),
            pltpu.VMEM((8 * 1024, 128), F32),
            pltpu.VMEM((8,) + share, F32),
            pltpu.VMEM((7, 2, 256, 256), BF16),
            pltpu.VMEM((8, 2) + share, F32),
            pltpu.VMEM((8, 2) + share, F32),
            pltpu.VMEM((8, 2) + share, F32),
            pltpu.VMEM((8, 4) + share, F32),
            pltpu.VMEM((8, 4) + share, F32),
            pltpu.VMEM((2, 512, 128), F32),
            pltpu.VMEM((DEVICES * 8, 128), F32),
            pltpu.VMEM((DEVICES * 16, 128), F32),
            pltpu.VMEM((5, 128, 128), F32),
            pltpu.VMEM((128, 128), F32),
            pltpu.VMEM((1, 1, 128), F32),
            pltpu.VMEM((32, N), jnp.int32),
            pltpu.VMEM((5, 128, 128), F32),
            pltpu.VMEM((4, 128, 128), F32),
            pltpu.VMEM((4, 128, 128), F32),
            pltpu.VMEM((128, 128), F32),
            dma((8,)),
            dma,
            dma,
            dma((4,)),
            dma((80,)),
            dma((80,)),
            dma((8,)),
        ],
        compiler_params=params(collective_id=0, has_side_effects=True),
    )(density, lens_weight, spectrum_bin.T, mats)
    real, imag, spectrum = pl.pallas_call(
        finish,
        name="finish",
        out_shape=shapes,
        in_specs=[vmem, vmem, vmem],
        out_specs=(hbm, hbm, hbm),
        scratch_shapes=[dma((3,))],
        compiler_params=params(),
    )(*results)
    return real, imag, spectrum.reshape(NBINS)


def solution(mesh):
    finer = Mesh(mesh.devices.reshape(4, 2, 2, 4, 2), AXES)
    tables = jnp.asarray(make_tables())
    step = jax.shard_map(
        on_device,
        mesh=finer,
        in_specs=(P(), P(PLANES, ROWS, None), P(PLANES), P(None, AXES)),
        out_specs=(P(AXES, None), P(AXES, None), P()),
        check_vma=False,
    )

    def whole(density, lens_weight, spectrum_bin):
        return step(tables, density, lens_weight, spectrum_bin)

    return whole
```

```python
from functools import partial
import math

import jax
import jax.numpy as jnp
import ml_dtypes
import numpy as np
from jax import lax
from jax.experimental import pallas as pl
from jax.experimental.pallas import tpu as pltpu
from jax.sharding import Mesh
from jax.sharding import PartitionSpec as P

N = 4096
NBINS = 64
DEVICES = 128
AXES = ("x", "zl", "core", "y", "zh")
ROWS = ("x", "zl", "core")
PLANES = ("y", "zh")
LOGICAL = pl.DeviceIdType.LOGICAL
F32 = jnp.float32
BF16 = jnp.bfloat16


def halves(table):
    high = table.astype(np.float32).astype(ml_dtypes.bfloat16)
    low = (table - high.astype(np.float64)).astype(np.float32).astype(ml_dtypes.bfloat16)
    return np.stack([high, low])


def make_tables():
    turn = 2.0 * math.pi
    i128 = np.arange(128)
    angle = turn * ((i128[:, None] * i128[None, :]) % 128) / 128
    cos, sin = np.cos(angle), np.sin(angle)
    forward = np.block([[cos, sin], [-sin, cos]])
    inverse = np.block([[cos, -sin], [sin, cos]])
    first = np.zeros((256, 256))
    back = np.zeros((256, 256))
    for d in range(128):
        if d < 64:
            phase = turn * (((16 + 32 * d) * i128) % 4096) / 4096
            first[d, 128:] = np.cos(phase)
            first[128 + d, 128:] = -np.sin(phase)
            weight = 2.0
        elif d == 64:
            first[d, :128] = 1.0
            first[128 + d, :128] = (-1.0) ** i128
            weight = 1.0
        else:
            phase = turn * ((d * i128) % 128) / 128
            first[d, :128] = np.cos(phase)
            first[128 + d, :128] = -np.sin(phase)
            weight = 2.0
        back[:, d] = weight * first[d]
        back[:, 128 + d] = weight * first[128 + d]
    small = np.zeros((4, 32, 32, 4), np.complex128)
    i32 = np.arange(32)
    kernel = np.exp(-1j * turn * ((i32[:, None] * i32[None, :]) % 32) / 32)
    for c in range(4):
        small[c, :, :, c] = kernel
    small = small.reshape(128, 128)
    lanes = np.block([[small.real, small.imag], [-small.imag, small.real]])
    wide = np.conj(small).T
    lanes_back = np.block([[wide.real, wide.imag], [-wide.imag, wide.real]])
    mats = np.stack([halves(t) for t in (forward, inverse, first, back, lanes, lanes_back)])
    y2 = np.tile(i32, 4)
    phase = turn * (i128[:, None] * y2[None, :]) / 4096
    column_twiddle = np.stack([np.cos(phase), np.sin(phase)]).astype(np.float32)
    phase = turn * (np.arange(16)[:, None] * i128[None, :]) / 4096
    row_twiddle = np.stack([np.cos(phase), np.sin(phase)]).astype(np.float32)
    extra = np.zeros((1, 2, 256, 256), ml_dtypes.bfloat16)
    for c in range(2):
        for j, (up, left) in enumerate(((0, 0), (0, 128), (128, 0))):
            part = column_twiddle[c].astype(ml_dtypes.bfloat16)
            column_twiddle[c] -= part.astype(np.float32)
            extra[0, c, up : up + 128, left : left + 128] = part
            part = row_twiddle[c].astype(ml_dtypes.bfloat16)
            row_twiddle[c] -= part.astype(np.float32)
            extra[0, c, 128 + 16 * j : 144 + 16 * j, 128:] = part
    return np.concatenate([mats, extra])


FORWARD, INVERSE, FIRST, BACK, LANES, LANES_BACK, TWIDDLES = range(7)


def rfft(values):
    n = len(values)
    if n == 2:
        return [(values[0] + values[1], None), (values[0] - values[1], None)]
    even, odd = rfft(values[0::2]), rfft(values[1::2])
    out = [None] * (n // 2 + 1)
    out[0] = (even[0][0] + odd[0][0], None)
    out[n // 2] = (even[0][0] - odd[0][0], None)
    for k in range(1, n // 4):
        c, s = math.cos(2 * math.pi * k / n), math.sin(2 * math.pi * k / n)
        er, ei = even[k]
        orr, oi = odd[k]
        if 8 * k == n:
            pr, pi = (orr + oi) * c, (oi - orr) * c
        else:
            pr, pi = orr * c + oi * s, oi * c - orr * s
        out[k] = (er + pr, ei + pi)
        out[n // 2 - k] = (er - pr, pi - ei)
    out[n // 4] = (even[n // 4][0], -odd[n // 4][0])
    return out


def irfft(g):
    n = 2 * (len(g) - 1)
    if n == 2:
        return [g[0][0] + g[1][0], g[0][0] - g[1][0]]
    even, odd = [None] * (n // 4 + 1), [None] * (n // 4 + 1)
    even[0] = (g[0][0] + g[n // 2][0], None)
    odd[0] = (g[0][0] - g[n // 2][0], None)
    for k in range(1, n // 4):
        c, s = math.cos(2 * math.pi * k / n), math.sin(2 * math.pi * k / n)
        ar, ai = g[k]
        br, bi = g[n // 2 - k]
        even[k] = (ar + br, ai - bi)
        dr, di = ar - br, ai + bi
        odd[k] = (dr * c - di * s, dr * s + di * c)
    mr, mi = g[n // 4]
    even[n // 4] = (mr + mr, None)
    odd[n // 4] = (-(mi + mi), None)
    a, b = irfft(even), irfft(odd)
    out = [None] * n
    out[0::2], out[1::2] = a, b
    return out


def split(value):
    high = value.astype(BF16)
    return high, (value - high.astype(F32)).astype(BF16)


def table_times(mats, which, data):
    high, low = split(data)
    dot = partial(jnp.dot, preferred_element_type=F32)
    return dot(mats[which, 0], high) + dot(mats[which, 0], low) + dot(mats[which, 1], high)


def times_table(mats, which, data):
    high, low = split(data)
    dot = partial(jnp.dot, preferred_element_type=F32)
    return dot(high, mats[which, 0]) + dot(low, mats[which, 0]) + dot(high, mats[which, 1])


def read_twiddles(mats, ctw, rtw):
    for c in range(2):
        parts = [
            mats[TWIDDLES, c, pl.ds(up, 128), pl.ds(left, 128)].astype(F32)
            for up, left in ((0, 0), (0, 128), (128, 0))
        ]
        ctw[c] = parts[0] + parts[1] + parts[2]
        parts = [
            mats[TWIDDLES, c, pl.ds(128 + 16 * j, 16), pl.ds(128, 128)].astype(F32)
            for j in range(3)
        ]
        rtw[c] = parts[0] + parts[1] + parts[2]


def my_index():
    x, zl, core, y, zh = (lax.axis_index(a) for a in AXES)
    return ((x * 2 + zl) * 2 + core) * 8 + y * 2 + zh


def row_forward(b, w, mine, mats, rtw, ubuf, spread):
    for q in range(4):
        rows = pl.ds(b * 32 + q * 8, 8)
        out = rfft([mine[rows, pl.ds(x1 * 128, 128)] * w for x1 in range(32)])
        for k1 in range(16):
            at = pl.ds(k1 * 32 + q * 8, 8)
            if k1 == 0:
                ubuf[0, at, :], ubuf[1, at, :] = out[0][0], out[16][0]
            else:
                tr, ti = rtw[0, pl.ds(k1, 1), :], rtw[1, pl.ds(k1, 1), :]
                ur, ui = out[k1]
                ubuf[0, at, :] = ur * tr + ui * ti
                ubuf[1, at, :] = ui * tr - ur * ti
    data = jnp.concatenate([ubuf[0].T, ubuf[1].T], axis=0)
    out = table_times(mats, FORWARD, data)
    special = table_times(mats, FIRST, data[:, :128])
    lane = lax.broadcasted_iota(jnp.int32, (256, 128), 1)
    for t in range(4):
        piece = out[:, t * 128 : (t + 1) * 128]
        if t == 0:
            piece = jnp.where(lane < 32, special, piece)
        for c in range(2):
            for r in range(16):
                at = c * 128 + r * 8
                spread[pl.ds(b * 1024 + r * 8 + c * 4 + t, 8, stride=128), :] = piece[at : at + 8]


def column_part(me, recv, mats, ctw, power, msg, send):
    lane = lax.broadcasted_iota(jnp.int32, (128, 128), 1)
    sub = lax.broadcasted_iota(jnp.int32, (128, 128), 0)
    special = jnp.logical_and(lane < 32, me == 64)
    re = [recv[pl.ds(t, 128, stride=8), :] for t in range(4)]
    im = [recv[pl.ds(4 + t, 128, stride=8), :] for t in range(4)]
    zero = jnp.zeros((128, 128), F32)
    re.append(jnp.where(special, im[0], zero))
    im[0] = jnp.where(special, zero, im[0])
    im.append(zero)
    data = jnp.concatenate([jnp.concatenate(re, axis=1), jnp.concatenate(im, axis=1)], axis=0)
    y = table_times(mats, FORWARD, data)
    tc, ts = ctw[0], ctw[1]
    rows = []
    for t in range(5):
        yr, yi = y[:128, t * 128 : (t + 1) * 128], y[128:, t * 128 : (t + 1) * 128]
        rows.append(jnp.concatenate([yr * tc + yi * ts, yi * tc - yr * ts], axis=1))
    f = times_table(mats, LANES, jnp.concatenate(rows, axis=0))
    ky2 = lane // 4
    col = lane % 4
    ky = sub + 128 * ky2
    nyquist = ky == 2048
    ky = jnp.where(ky >= 2048, ky - 4096, ky).astype(F32)
    scale = 1.0 / (float(N) * float(N))
    hats = []
    for t in range(5):
        fr, fi = f[t * 128 : (t + 1) * 128, :128], f[t * 128 : (t + 1) * 128, 128:]
        if t < 4:
            slot = t * 4 + col
            kx = slot + 32 * me
            if t == 0:
                zeroth = jnp.where(
                    me < 64, 16 + 32 * me, jnp.where(me == 64, 0, 32 * me)
                )
                kx = jnp.where(slot == 0, zeroth, kx)
            kx = jnp.where(kx >= 2048, kx - 4096, kx).astype(F32)
        else:
            kx = jnp.full((128, 128), -2048.0, F32)
        norm = kx * kx + ky * ky
        if t == 0:
            anchor = norm == 0
            norm = jnp.where(anchor, 1.0, norm)
            fr, fi = jnp.where(anchor, 0.0, fr), jnp.where(anchor, 0.0, fi)
        power[t] = fr * fr + fi * fi
        inv = scale / norm
        kr = (kx * kx - ky * ky) * inv
        ki = 2.0 * kx * ky * inv
        if t < 4:
            kn = jnp.where(nyquist, ki, 0.0)
            ki = jnp.where(nyquist, 0.0, ki)
            a = (kr * fr - kn * fi, kr * fi + kn * fr)
            c = (ki * fr, ki * fi)
        else:
            kn = jnp.where(nyquist, ki, 0.0)
            ki = jnp.where(nyquist, 0.0, ki)
            a = (kr * fr - ki * fi, kr * fi + ki * fr)
            c = (kn * fr, kn * fi)
        hats.append((a, c))
    for ac in range(2):
        rows = [jnp.concatenate(hats[t][ac], axis=1) for t in range(5)]
        g = times_table(mats, LANES_BACK, jnp.concatenate(rows, axis=0))
        re, im = [], []
        for t in range(5):
            gr, gi = g[t * 128 : (t + 1) * 128, :128], g[t * 128 : (t + 1) * 128, 128:]
            re.append(gr * tc - gi * ts)
            im.append(gi * tc + gr * ts)
        data = jnp.concatenate([jnp.concatenate(re, axis=1), jnp.concatenate(im, axis=1)], axis=0)
        s = table_times(mats, INVERSE, data)
        for t in range(4):
            sr, si = s[:128, t * 128 : (t + 1) * 128], s[128:, t * 128 : (t + 1) * 128]
            if t == 0:
                si = jnp.where(special, s[:128, 512:], si)
            msg[pl.ds(ac * 1024 + t, 128, stride=8), :] = sr
            msg[pl.ds(ac * 1024 + 4 + t, 128, stride=8), :] = si
        send(ac)


def row_inverse(ac, recv, mats, rtw, vbuf, out_ref):
    lane = lax.broadcasted_iota(jnp.int32, (256, 128), 1)
    parts = [
        jnp.concatenate(
            [recv[pl.ds(ac * 1024 + c * 4 + t, 128, stride=8), :] for t in range(4)], axis=1
        )
        for c in range(2)
    ]
    data = jnp.concatenate(parts, axis=0)
    v = table_times(mats, INVERSE, data)
    special = table_times(mats, BACK, data[:, :128])
    first = jnp.where(lane < 32, special, v[:, :128])
    for c in range(2):
        rows = slice(c * 128, (c + 1) * 128)
        full = jnp.concatenate([first[rows], v[rows, 128:]], axis=1)
        vbuf[c] = full.T
    for q in range(4):
        g = [None] * 17
        for k1 in range(16):
            at = pl.ds(k1 * 32 + q * 8, 8)
            vr, vi = vbuf[0, at, :], vbuf[1, at, :]
            if k1 == 0:
                g[0], g[16] = (vr, None), (vi, None)
            else:
                tr, ti = rtw[0, pl.ds(k1, 1), :], rtw[1, pl.ds(k1, 1), :]
                g[k1] = (vr * tr - vi * ti, vi * tr + vr * ti)
        out = irfft(g)
        for x1 in range(32):
            out_ref[pl.ds(q * 8, 8), pl.ds(x1 * 128, 128)] = out[x1]


STRIDE = 107


def peer(me, i):
    return lax.rem(me + i * STRIDE, DEVICES)


def send_all(me, half, msg, recv, send, arrive):
    def block(d):
        return pl.ds(pl.multiple_of((half * DEVICES + d) * 8, 8), 8)

    def step(i, _):
        to = peer(me, i)
        pltpu.make_async_remote_copy(
            src_ref=msg.at[block(to)],
            dst_ref=recv.at[block(me)],
            send_sem=send,
            recv_sem=arrive,
            device_id=to,
            device_id_type=LOGICAL,
        ).start()
        return 0

    lax.fori_loop(1, DEVICES, step, 0)
    recv[block(me), :] = msg[block(me), :]


def wait_all(buf, sem, rows, count=DEVICES - 1):
    part = buf.at[pl.ds(0, count * rows)]
    pltpu.make_async_copy(part, part, sem).wait()


def arrange_bins(me, raw, near, far):
    row = lax.broadcasted_iota(jnp.int32, (128, 128), 0)
    lane = lax.broadcasted_iota(jnp.int32, (128, 128), 1)
    rcol, rky2 = row % 32, row // 32
    lcol, lky2 = lane % 4, lane // 4
    low = me < 64
    wanted = []
    for t in range(4):
        slot = 4 * t + lcol
        own, other = slot, 32 - slot
        if t == 0:
            own = jnp.where(slot == 0, jnp.where(low, 16, 0), own)
            other = jnp.where(slot == 0, jnp.where(low, 0, 16), other)
        wanted.append((rcol == own, lky2 - rky2))
        wanted.append((rcol == other, 31 - lky2 - rky2))
    wanted.append((jnp.logical_and(lcol == 0, rcol == 0), lky2 - rky2))
    sums = [jnp.zeros((128, 128), F32) for _ in wanted]
    for g in range(8):
        pieces = [raw[:, pl.ds((4 * g + i) * 128, 128)].astype(F32) for i in range(4)]
        data = jnp.concatenate(pieces, axis=0).T.astype(BF16)
        for i, (match, shift) in enumerate(wanted):
            pick = jnp.where(jnp.logical_and(match, shift == 4 * g), 1.0, 0.0).astype(BF16)
            sums[i] = sums[i] + jnp.dot(data, pick, preferred_element_type=F32)
    flip = jnp.where(jnp.logical_and(row + lane == 128, row > 0), 1.0, 0.0).astype(BF16)
    for t in range(4):
        own, other = sums[2 * t], sums[2 * t + 1]
        if t == 0:
            own = jnp.where(jnp.logical_and(lcol == 0, me == 64), float(NBINS), own)
        near[t] = own
        turned = jnp.dot(flip, other.astype(BF16), preferred_element_type=F32)
        first = jnp.concatenate([other[:1, 124:], other[:1, :124]], axis=1)
        far[t] = jnp.where(row == 0, first, turned)
    near[4] = sums[8]


def bin_power(near, far, power, acc, spec):
    def group(g, _):
        sums = [jnp.zeros((8, 128), F32) for _ in range(8)]
        for i in range(9):
            t = i % 5 if i < 5 else i - 5
            which = 0 if i < 5 else 1
            for r in range(16):
                at = pl.ds(r * 8, 8)
                b = (far if which else near)[t, at, :] - (g * 8).astype(F32)
                p = power[t, at, :]
                for k in range(8):
                    sums[k] = sums[k] + jnp.where(b == float(k), p, 0.0)
        rows = [jnp.sum(v, axis=0, keepdims=True) for v in sums]
        acc[pl.ds(pl.multiple_of(g * 8, 8), 8), :] = jnp.concatenate(rows, axis=0)
        return 0

    lax.fori_loop(0, 8, group, 0)
    acc[pl.ds(64, 64), :] = jnp.zeros((64, 128), F32)
    row = jnp.sum(acc[...].T, axis=0, keepdims=True)
    spec[0] = row * (NBINS / float(N) ** 4)


class Reduction:
    def __init__(self, spread, total, yrelay, ydirect, yfinal, zrecv, zsum, ssem, rsem):
        self.spread, self.total, self.zrecv, self.zsum = spread, total, zrecv, zsum
        self.yrelay, self.ydirect, self.yfinal = yrelay, ydirect, yfinal
        self.ssem, self.rsem, self.sends = ssem, rsem, []
        y, zh = lax.axis_index("y"), lax.axis_index("zh")
        base = my_index() - y * 2 - zh
        up, down, across = lax.rem(y + 1, 4), lax.rem(y + 3, 4), lax.rem(y + 2, 4)
        self.y, self.zh, self.turn = y, zh, (across, up, down, y)
        self.dev_up, self.dev_down = base + up * 2 + zh, base + down * 2 + zh
        self.dev_z = base + y * 2 + (1 - zh)
        self.moves = {}

    def send(self, key, src, dst, to):
        i = len(self.sends)
        copy = pltpu.make_async_remote_copy(
            src_ref=src,
            dst_ref=dst,
            send_sem=self.ssem.at[i],
            recv_sem=self.rsem.at[i],
            device_id=to,
            device_id_type=LOGICAL,
        )
        copy.start()
        self.sends.append(copy)
        self.moves[key] = copy

    def arrived(self, *keys):
        for key in keys:
            self.moves[key].wait_recv()

    def share(self, t, h, b):
        return self.spread.at[pl.ds(pl.multiple_of(b * 1024 + (t * 2 + h) * 128, 128), 128)]


    def y_start(self, b):
        across, up, down, _ = self.turn
        self.send(("relay", b, 0), self.share(across, 0, b), self.yrelay.at[b, 0], self.dev_up)
        self.send(("relay", b, 1), self.share(across, 1, b), self.yrelay.at[b, 1], self.dev_down)
        self.send(("direct", b, 0), self.share(up, 1, b), self.ydirect.at[b, 1], self.dev_up)
        self.send(("direct", b, 1), self.share(down, 0, b), self.ydirect.at[b, 0], self.dev_down)

    def y_relay(self, b):
        for h, t, to in ((0, self.turn[1], self.dev_up), (1, self.turn[2], self.dev_down)):
            self.arrived(("relay", b, h))
            self.yrelay[b, h] = self.yrelay[b, h] + self.share(t, h, b)[...]
            self.send(("final", b, h), self.yrelay.at[b, h], self.yfinal.at[b, h], to)

    def y_finish(self, b):
        self.arrived(("direct", b, 0), ("direct", b, 1), ("final", b, 0), ("final", b, 1))
        for h in range(2):
            own = self.share(self.y, h, b)[...]
            self.yfinal[b, h] = self.yfinal[b, h] + self.ydirect[b, h] + own
        self.send(("z", b, 0), self.yfinal.at[b, 1 - self.zh], self.zrecv.at[b, 0], self.dev_z)

    def z_last(self, b):
        self.arrived(("z", b, 0))
        self.total[b] = self.zrecv[b, 0] + self.yfinal[b, self.zh]


    def z_start(self, b):
        for i, t in enumerate(self.turn):
            self.send(("z", b, i), self.share(t, 1 - self.zh, b), self.zrecv.at[b, i], self.dev_z)

    def z_then_y(self, b):
        low, high = pl.ds(0, 64), pl.ds(64, 64)
        zsum = self.zsum
        for i, t in enumerate(self.turn):
            self.arrived(("z", b, i))
            zsum[b, i] = self.zrecv[b, i] + self.share(t, self.zh, b)[...]
            if i == 0:
                up, down = self.yrelay.at[b, 0, low], self.yrelay.at[b, 1, low]
                self.send(("relay", b, 0), zsum.at[b, 0, low], up, self.dev_up)
                self.send(("relay", b, 1), zsum.at[b, 0, high], down, self.dev_down)
            if i == 1:
                up = self.ydirect.at[b, 1, low]
                self.send(("direct", b, 0), zsum.at[b, 1, high], up, self.dev_up)
            if i == 2:
                down = self.ydirect.at[b, 0, low]
                self.send(("direct", b, 1), zsum.at[b, 2, low], down, self.dev_down)

    def y_relay_half(self, b):
        low = pl.ds(0, 64)
        for h, i, to in ((0, 1, self.dev_up), (1, 2, self.dev_down)):
            self.arrived(("relay", b, h))
            own = self.zsum[b, i, pl.ds(h * 64, 64)]
            self.yrelay[b, h, low] = self.yrelay[b, h, low] + own
            self.send(("final", b, h), self.yrelay.at[b, h, low], self.yfinal.at[b, h, low], to)

    def y_last(self, b):
        self.arrived(("direct", b, 0), ("direct", b, 1), ("final", b, 0), ("final", b, 1))
        low = pl.ds(0, 64)
        for h in range(2):
            rows = pl.ds(h * 64, 64)
            new = self.yfinal[b, h, low] + self.ydirect[b, h, low]
            self.total[b, rows] = self.zsum[b, 3, rows] + new


def kernel(
    density, weight, bins_in, mats_in, out_real, out_imag, out_spec,
    recvc, specs, ctw, rtw, mine, spread, total, mats, yrelay, ydirect, yfinal, zrecv, zsum,
    ubuf, recvb, msgc, power, acc, spec, raw, near, far, farin, extra,
    lsem, msem, bsem, fsem, ssem, rsem, asem,
):
    me = my_index()
    barrier = pltpu.get_barrier_semaphore()
    loads = []
    for i in range(8):
        copy = pltpu.make_async_copy(
            density.at[0, pl.ds(i * 32, 32)], mine.at[pl.ds(i * 32, 32)], lsem.at[i]
        )
        copy.start()
        loads.append(copy)
    mload = pltpu.make_async_copy(mats_in, mats, msem)
    mload.start()
    bload = pltpu.make_async_copy(bins_in, raw, bsem)
    bload.start()

    def greet(i, _):
        pl.semaphore_signal(
            barrier, inc=1, device_id=lax.rem(me + i, DEVICES), device_id_type=LOGICAL
        )
        return 0

    lax.fori_loop(1, DEVICES, greet, 0)
    w = weight[0]
    mload.wait()
    read_twiddles(mats, ctw, rtw)
    row, plane = me // 8, lax.rem(me, 8)
    red = Reduction(spread, total, yrelay, ydirect, yfinal, zrecv, zsum, ssem, rsem)

    def transform(b):
        loads[b].wait()
        row_forward(b, w, mine, mats, rtw, ubuf, spread)

    def to_columns(b):
        at = pl.ds(pl.multiple_of((row * 8 + b) * 8, 8), 8)

        def step(i, _):
            to = lax.rem(row + i * 5, 16)
            pltpu.make_async_remote_copy(
                src_ref=total.at[b, pl.ds(pl.multiple_of(to * 8, 8), 8)],
                dst_ref=recvb.at[at],
                send_sem=asem.at[0],
                recv_sem=asem.at[1],
                device_id=to * 8 + plane,
                device_id_type=LOGICAL,
            ).start()
            return 0

        lax.fori_loop(1, 16, step, 0)
        recvb[at, :] = total[b, pl.ds(pl.multiple_of(row * 8, 8), 8), :]

    transform(5)
    transform(0)
    pl.semaphore_wait(barrier, DEVICES - 1)
    red.z_start(5)
    red.y_start(0)
    transform(6)
    red.z_start(6)
    transform(1)
    red.y_start(1)
    red.y_relay(0)
    transform(7)
    red.z_start(7)
    transform(2)
    red.y_start(2)
    red.y_relay(1)
    transform(3)
    transform(4)
    red.z_then_y(5)
    red.y_start(3)
    red.y_relay(2)
    red.y_finish(0)
    red.y_relay_half(5)
    bload.wait()
    arrange_bins(me, raw, near, far)
    red.y_start(4)
    red.y_relay(3)
    red.y_finish(1)
    red.z_then_y(6)
    red.y_relay(4)
    red.y_relay_half(6)
    red.y_finish(2)
    red.y_last(5)
    to_columns(5)
    red.z_last(0)
    to_columns(0)
    red.y_finish(3)
    red.z_then_y(7)
    red.z_last(1)
    to_columns(1)
    red.y_relay_half(7)
    red.y_finish(4)
    red.y_last(6)
    to_columns(6)
    red.z_last(2)
    to_columns(2)
    red.z_last(3)
    to_columns(3)
    red.y_last(7)
    to_columns(7)
    red.z_last(4)
    to_columns(4)
    mirror = pltpu.make_async_remote_copy(
        src_ref=far,
        dst_ref=farin,
        send_sem=fsem.at[0],
        recv_sem=fsem.at[1],
        device_id=DEVICES - 1 - me,
        device_id_type=LOGICAL,
    )
    mirror.start()
    zeroth = pltpu.make_async_remote_copy(
        src_ref=far.at[0],
        dst_ref=extra,
        send_sem=fsem.at[2],
        recv_sem=fsem.at[3],
        device_id=jnp.where(me == 0, 64, DEVICES - me),
        device_id_type=LOGICAL,
    )

    @pl.when(me < 64)
    def _():
        zeroth.start()

    wait_all(recvb, asem.at[1], 8, 120)

    def to_rows(ac):
        send_all(me, ac, msgc, recvc, asem.at[2 + ac], asem.at[6 + ac])

    column_part(me, recvb, mats, ctw, power, msgc, to_rows)
    mirror.wait_recv()

    @pl.when(me >= 64)
    def _():
        zeroth.wait_recv()
        lane = lax.broadcasted_iota(jnp.int32, (128, 128), 1)
        farin[0] = jnp.where(lane % 4 == 0, extra[...], farin[0])

    bin_power(near, farin, power, acc, spec)

    def share_spec(i, _):
        to = peer(me, i)
        pltpu.make_async_remote_copy(
            src_ref=spec.at[0],
            dst_ref=specs.at[me],
            send_sem=asem.at[4],
            recv_sem=asem.at[5],
            device_id=to,
            device_id_type=LOGICAL,
        ).start()
        return 0

    lax.fori_loop(1, DEVICES, share_spec, 0)
    specs[me] = spec[0]
    wait_all(recvc, asem.at[6], 8)
    row_inverse(0, recvc, mats, rtw, ubuf, out_real)
    wait_all(recvc, asem.at[7], 8)
    row_inverse(1, recvc, mats, rtw, ubuf, out_imag)
    wait_all(specs, asem.at[5], 1)
    power_sum = specs[0]
    for i in range(1, DEVICES):
        power_sum = power_sum + specs[i]
    out_spec[...] = power_sum[:, :NBINS]
    wait_all(recvb, asem.at[0], 8, 120)
    wait_all(msgc, asem.at[2], 8)
    wait_all(msgc, asem.at[3], 8)
    wait_all(specs, asem.at[4], 1)
    for copy in red.sends:
        copy.wait_send()
    mirror.wait_send()

    @pl.when(me < 64)
    def _():
        zeroth.wait_send()


def finish(*refs):
    sems = refs[6]
    copies = [pltpu.make_async_copy(refs[i], refs[3 + i], sems.at[i]) for i in range(3)]
    for copy in copies:
        copy.start()
    for copy in copies:
        copy.wait()


def on_device(mats, density, lens_weight, spectrum_bin):
    vmem = pl.BlockSpec(memory_space=pltpu.VMEM)
    hbm = pl.BlockSpec(memory_space=pltpu.HBM)
    smem = pl.BlockSpec(memory_space=pltpu.SMEM)
    dma = pltpu.SemaphoreType.DMA
    share = (128, 128)
    params = partial(pltpu.CompilerParams, vmem_limit_bytes=55050240)
    shapes = (
        jax.ShapeDtypeStruct((32, N), F32),
        jax.ShapeDtypeStruct((32, N), F32),
        jax.ShapeDtypeStruct((1, NBINS), F32),
    )
    results = pl.pallas_call(
        kernel,
        name="shear",
        out_shape=shapes,
        in_specs=[hbm, smem, hbm, hbm],
        out_specs=(vmem, vmem, vmem),
        scratch_shapes=[
            pltpu.VMEM((DEVICES * 16, 128), F32),
            pltpu.VMEM((DEVICES, 1, 128), F32),
            pltpu.VMEM((2, 128, 128), F32),
            pltpu.VMEM((2, 16, 128), F32),
            pltpu.VMEM((256, N), F32),
            pltpu.VMEM((8 * 1024, 128), F32),
            pltpu.VMEM((8,) + share, F32),
            pltpu.VMEM((7, 2, 256, 256), BF16),
            pltpu.VMEM((8, 2) + share, F32),
            pltpu.VMEM((8, 2) + share, F32),
            pltpu.VMEM((8, 2) + share, F32),
            pltpu.VMEM((8, 4) + share, F32),
            pltpu.VMEM((8, 4) + share, F32),
            pltpu.VMEM((2, 512, 128), F32),
            pltpu.VMEM((DEVICES * 8, 128), F32),
            pltpu.VMEM((DEVICES * 16, 128), F32),
            pltpu.VMEM((5, 128, 128), F32),
            pltpu.VMEM((128, 128), F32),
            pltpu.VMEM((1, 1, 128), F32),
            pltpu.VMEM((32, N), jnp.int32),
            pltpu.VMEM((5, 128, 128), F32),
            pltpu.VMEM((4, 128, 128), F32),
            pltpu.VMEM((4, 128, 128), F32),
            pltpu.VMEM((128, 128), F32),
            dma((8,)),
            dma,
            dma,
            dma((4,)),
            dma((80,)),
            dma((80,)),
            dma((8,)),
        ],
        compiler_params=params(collective_id=0, has_side_effects=True),
    )(density, lens_weight, spectrum_bin.T, mats)
    real, imag, spectrum = pl.pallas_call(
        finish,
        name="finish",
        out_shape=shapes,
        in_specs=[vmem, vmem, vmem],
        out_specs=(hbm, hbm, hbm),
        scratch_shapes=[dma((3,))],
        compiler_params=params(),
    )(*results)
    return real, imag, spectrum.reshape(NBINS)


def solution(mesh):
    finer = Mesh(mesh.devices.reshape(4, 2, 2, 4, 2), AXES)
    tables = jnp.asarray(make_tables())
    step = jax.shard_map(
        on_device,
        mesh=finer,
        in_specs=(P(), P(PLANES, ROWS, None), P(PLANES), P(None, AXES)),
        out_specs=(P(AXES, None), P(AXES, None), P()),
        check_vma=False,
    )

    def whole(density, lens_weight, spectrum_bin):
        return step(tables, density, lens_weight, spectrum_bin)

    return whole
```

```python
from functools import partial
import math

import jax
import jax.numpy as jnp
import ml_dtypes
import numpy as np
from jax import lax
from jax.experimental import pallas as pl
from jax.experimental.pallas import tpu as pltpu
from jax.sharding import Mesh
from jax.sharding import PartitionSpec as P

N = 4096
NBINS = 64
DEVICES = 128
AXES = ("x", "zl", "core", "y", "zh")
ROWS = ("x", "zl", "core")
PLANES = ("y", "zh")
LOGICAL = pl.DeviceIdType.LOGICAL
F32 = jnp.float32
BF16 = jnp.bfloat16


def halves(table):
    high = table.astype(np.float32).astype(ml_dtypes.bfloat16)
    low = (table - high.astype(np.float64)).astype(np.float32).astype(ml_dtypes.bfloat16)
    return np.stack([high, low])


def make_tables():
    turn = 2.0 * math.pi
    i128 = np.arange(128)
    angle = turn * ((i128[:, None] * i128[None, :]) % 128) / 128
    cos, sin = np.cos(angle), np.sin(angle)
    forward = np.block([[cos, sin], [-sin, cos]])
    inverse = np.block([[cos, -sin], [sin, cos]])
    first = np.zeros((256, 256))
    back = np.zeros((256, 256))
    for d in range(128):
        if d < 64:
            phase = turn * (((16 + 32 * d) * i128) % 4096) / 4096
            first[d, 128:] = np.cos(phase)
            first[128 + d, 128:] = -np.sin(phase)
            weight = 2.0
        elif d == 64:
            first[d, :128] = 1.0
            first[128 + d, :128] = (-1.0) ** i128
            weight = 1.0
        else:
            phase = turn * ((d * i128) % 128) / 128
            first[d, :128] = np.cos(phase)
            first[128 + d, :128] = -np.sin(phase)
            weight = 2.0
        back[:, d] = weight * first[d]
        back[:, 128 + d] = weight * first[128 + d]
    small = np.zeros((4, 32, 32, 4), np.complex128)
    i32 = np.arange(32)
    kernel = np.exp(-1j * turn * ((i32[:, None] * i32[None, :]) % 32) / 32)
    for c in range(4):
        small[c, :, :, c] = kernel
    small = small.reshape(128, 128)
    lanes = np.block([[small.real, small.imag], [-small.imag, small.real]])
    wide = np.conj(small).T
    lanes_back = np.block([[wide.real, wide.imag], [-wide.imag, wide.real]])
    mats = np.stack([halves(t) for t in (forward, inverse, first, back, lanes, lanes_back)])
    y2 = np.tile(i32, 4)
    phase = turn * (i128[:, None] * y2[None, :]) / 4096
    column_twiddle = np.stack([np.cos(phase), np.sin(phase)]).astype(np.float32)
    phase = turn * (np.arange(16)[:, None] * i128[None, :]) / 4096
    row_twiddle = np.stack([np.cos(phase), np.sin(phase)]).astype(np.float32)
    extra = np.zeros((1, 2, 256, 256), ml_dtypes.bfloat16)
    for c in range(2):
        for j, (up, left) in enumerate(((0, 0), (0, 128), (128, 0))):
            part = column_twiddle[c].astype(ml_dtypes.bfloat16)
            column_twiddle[c] -= part.astype(np.float32)
            extra[0, c, up : up + 128, left : left + 128] = part
            part = row_twiddle[c].astype(ml_dtypes.bfloat16)
            row_twiddle[c] -= part.astype(np.float32)
            extra[0, c, 128 + 16 * j : 144 + 16 * j, 128:] = part
    return np.concatenate([mats, extra])


FORWARD, INVERSE, FIRST, BACK, LANES, LANES_BACK, TWIDDLES = range(7)


def rfft(values):
    n = len(values)
    if n == 2:
        return [(values[0] + values[1], None), (values[0] - values[1], None)]
    even, odd = rfft(values[0::2]), rfft(values[1::2])
    out = [None] * (n // 2 + 1)
    out[0] = (even[0][0] + odd[0][0], None)
    out[n // 2] = (even[0][0] - odd[0][0], None)
    for k in range(1, n // 4):
        c, s = math.cos(2 * math.pi * k / n), math.sin(2 * math.pi * k / n)
        er, ei = even[k]
        orr, oi = odd[k]
        if 8 * k == n:
            pr, pi = (orr + oi) * c, (oi - orr) * c
        else:
            pr, pi = orr * c + oi * s, oi * c - orr * s
        out[k] = (er + pr, ei + pi)
        out[n // 2 - k] = (er - pr, pi - ei)
    out[n // 4] = (even[n // 4][0], -odd[n // 4][0])
    return out


def irfft(g):
    n = 2 * (len(g) - 1)
    if n == 2:
        return [g[0][0] + g[1][0], g[0][0] - g[1][0]]
    even, odd = [None] * (n // 4 + 1), [None] * (n // 4 + 1)
    even[0] = (g[0][0] + g[n // 2][0], None)
    odd[0] = (g[0][0] - g[n // 2][0], None)
    for k in range(1, n // 4):
        c, s = math.cos(2 * math.pi * k / n), math.sin(2 * math.pi * k / n)
        ar, ai = g[k]
        br, bi = g[n // 2 - k]
        even[k] = (ar + br, ai - bi)
        dr, di = ar - br, ai + bi
        odd[k] = (dr * c - di * s, dr * s + di * c)
    mr, mi = g[n // 4]
    even[n // 4] = (mr + mr, None)
    odd[n // 4] = (-(mi + mi), None)
    a, b = irfft(even), irfft(odd)
    out = [None] * n
    out[0::2], out[1::2] = a, b
    return out


def split(value):
    high = value.astype(BF16)
    return high, (value - high.astype(F32)).astype(BF16)


def table_times(mats, which, data):
    high, low = split(data)
    dot = partial(jnp.dot, preferred_element_type=F32)
    return dot(mats[which, 0], high) + dot(mats[which, 0], low) + dot(mats[which, 1], high)


def times_table(mats, which, data):
    high, low = split(data)
    dot = partial(jnp.dot, preferred_element_type=F32)
    return dot(high, mats[which, 0]) + dot(low, mats[which, 0]) + dot(high, mats[which, 1])


def read_twiddles(mats, ctw, rtw):
    for c in range(2):
        parts = [
            mats[TWIDDLES, c, pl.ds(up, 128), pl.ds(left, 128)].astype(F32)
            for up, left in ((0, 0), (0, 128), (128, 0))
        ]
        ctw[c] = parts[0] + parts[1] + parts[2]
        parts = [
            mats[TWIDDLES, c, pl.ds(128 + 16 * j, 16), pl.ds(128, 128)].astype(F32)
            for j in range(3)
        ]
        rtw[c] = parts[0] + parts[1] + parts[2]


def my_index():
    x, zl, core, y, zh = (lax.axis_index(a) for a in AXES)
    return ((x * 2 + zl) * 2 + core) * 8 + y * 2 + zh


def row_forward(b, w, mine, mats, rtw, ubuf, spread):
    for q in range(4):
        rows = pl.ds(b * 32 + q * 8, 8)
        out = rfft([mine[rows, pl.ds(x1 * 128, 128)] * w for x1 in range(32)])
        for k1 in range(16):
            at = pl.ds(k1 * 32 + q * 8, 8)
            if k1 == 0:
                ubuf[0, at, :], ubuf[1, at, :] = out[0][0], out[16][0]
            else:
                tr, ti = rtw[0, pl.ds(k1, 1), :], rtw[1, pl.ds(k1, 1), :]
                ur, ui = out[k1]
                ubuf[0, at, :] = ur * tr + ui * ti
                ubuf[1, at, :] = ui * tr - ur * ti
    data = jnp.concatenate([ubuf[0].T, ubuf[1].T], axis=0)
    out = table_times(mats, FORWARD, data)
    special = table_times(mats, FIRST, data[:, :128])
    lane = lax.broadcasted_iota(jnp.int32, (256, 128), 1)
    for t in range(4):
        piece = out[:, t * 128 : (t + 1) * 128]
        if t == 0:
            piece = jnp.where(lane < 32, special, piece)
        for c in range(2):
            for r in range(16):
                at = c * 128 + r * 8
                spread[pl.ds(b * 1024 + r * 8 + c * 4 + t, 8, stride=128), :] = piece[at : at + 8]


def column_part(me, recv, mats, ctw, power, msg, send):
    lane = lax.broadcasted_iota(jnp.int32, (128, 128), 1)
    sub = lax.broadcasted_iota(jnp.int32, (128, 128), 0)
    special = jnp.logical_and(lane < 32, me == 64)
    re = [recv[pl.ds(t, 128, stride=8), :] for t in range(4)]
    im = [recv[pl.ds(4 + t, 128, stride=8), :] for t in range(4)]
    zero = jnp.zeros((128, 128), F32)
    re.append(jnp.where(special, im[0], zero))
    im[0] = jnp.where(special, zero, im[0])
    im.append(zero)
    data = jnp.concatenate([jnp.concatenate(re, axis=1), jnp.concatenate(im, axis=1)], axis=0)
    y = table_times(mats, FORWARD, data)
    tc, ts = ctw[0], ctw[1]
    rows = []
    for t in range(5):
        yr, yi = y[:128, t * 128 : (t + 1) * 128], y[128:, t * 128 : (t + 1) * 128]
        rows.append(jnp.concatenate([yr * tc + yi * ts, yi * tc - yr * ts], axis=1))
    f = times_table(mats, LANES, jnp.concatenate(rows, axis=0))
    ky2 = lane // 4
    col = lane % 4
    ky = sub + 128 * ky2
    nyquist = ky == 2048
    ky = jnp.where(ky >= 2048, ky - 4096, ky).astype(F32)
    scale = 1.0 / (float(N) * float(N))
    hats = []
    for t in range(5):
        fr, fi = f[t * 128 : (t + 1) * 128, :128], f[t * 128 : (t + 1) * 128, 128:]
        if t < 4:
            slot = t * 4 + col
            kx = slot + 32 * me
            if t == 0:
                zeroth = jnp.where(
                    me < 64, 16 + 32 * me, jnp.where(me == 64, 0, 32 * me)
                )
                kx = jnp.where(slot == 0, zeroth, kx)
            kx = jnp.where(kx >= 2048, kx - 4096, kx).astype(F32)
        else:
            kx = jnp.full((128, 128), -2048.0, F32)
        norm = kx * kx + ky * ky
        if t == 0:
            anchor = norm == 0
            norm = jnp.where(anchor, 1.0, norm)
            fr, fi = jnp.where(anchor, 0.0, fr), jnp.where(anchor, 0.0, fi)
        power[t] = fr * fr + fi * fi
        inv = scale / norm
        kr = (kx * kx - ky * ky) * inv
        ki = 2.0 * kx * ky * inv
        if t < 4:
            kn = jnp.where(nyquist, ki, 0.0)
            ki = jnp.where(nyquist, 0.0, ki)
            a = (kr * fr - kn * fi, kr * fi + kn * fr)
            c = (ki * fr, ki * fi)
        else:
            kn = jnp.where(nyquist, ki, 0.0)
            ki = jnp.where(nyquist, 0.0, ki)
            a = (kr * fr - ki * fi, kr * fi + ki * fr)
            c = (kn * fr, kn * fi)
        hats.append((a, c))
    for ac in range(2):
        rows = [jnp.concatenate(hats[t][ac], axis=1) for t in range(5)]
        g = times_table(mats, LANES_BACK, jnp.concatenate(rows, axis=0))
        re, im = [], []
        for t in range(5):
            gr, gi = g[t * 128 : (t + 1) * 128, :128], g[t * 128 : (t + 1) * 128, 128:]
            re.append(gr * tc - gi * ts)
            im.append(gi * tc + gr * ts)
        data = jnp.concatenate([jnp.concatenate(re, axis=1), jnp.concatenate(im, axis=1)], axis=0)
        s = table_times(mats, INVERSE, data)
        for t in range(4):
            sr, si = s[:128, t * 128 : (t + 1) * 128], s[128:, t * 128 : (t + 1) * 128]
            if t == 0:
                si = jnp.where(special, s[:128, 512:], si)
            msg[pl.ds(ac * 1024 + t, 128, stride=8), :] = sr
            msg[pl.ds(ac * 1024 + 4 + t, 128, stride=8), :] = si
        send(ac)


def row_inverse(ac, recv, mats, rtw, vbuf, out_ref):
    lane = lax.broadcasted_iota(jnp.int32, (256, 128), 1)
    parts = [
        jnp.concatenate(
            [recv[pl.ds(ac * 1024 + c * 4 + t, 128, stride=8), :] for t in range(4)], axis=1
        )
        for c in range(2)
    ]
    data = jnp.concatenate(parts, axis=0)
    v = table_times(mats, INVERSE, data)
    special = table_times(mats, BACK, data[:, :128])
    first = jnp.where(lane < 32, special, v[:, :128])
    for c in range(2):
        rows = slice(c * 128, (c + 1) * 128)
        full = jnp.concatenate([first[rows], v[rows, 128:]], axis=1)
        vbuf[c] = full.T
    for q in range(4):
        g = [None] * 17
        for k1 in range(16):
            at = pl.ds(k1 * 32 + q * 8, 8)
            vr, vi = vbuf[0, at, :], vbuf[1, at, :]
            if k1 == 0:
                g[0], g[16] = (vr, None), (vi, None)
            else:
                tr, ti = rtw[0, pl.ds(k1, 1), :], rtw[1, pl.ds(k1, 1), :]
                g[k1] = (vr * tr - vi * ti, vi * tr + vr * ti)
        out = irfft(g)
        for x1 in range(32):
            out_ref[pl.ds(q * 8, 8), pl.ds(x1 * 128, 128)] = out[x1]


STRIDE = 107


def peer(me, i):
    return lax.rem(me + i * STRIDE, DEVICES)


def send_all(me, half, msg, recv, send, arrive):
    def block(d):
        return pl.ds(pl.multiple_of((half * DEVICES + d) * 8, 8), 8)

    def step(i, _):
        to = peer(me, i)
        pltpu.make_async_remote_copy(
            src_ref=msg.at[block(to)],
            dst_ref=recv.at[block(me)],
            send_sem=send,
            recv_sem=arrive,
            device_id=to,
            device_id_type=LOGICAL,
        ).start()
        return 0

    lax.fori_loop(1, DEVICES, step, 0)
    recv[block(me), :] = msg[block(me), :]


def wait_all(buf, sem, rows, count=DEVICES - 1):
    part = buf.at[pl.ds(0, count * rows)]
    pltpu.make_async_copy(part, part, sem).wait()


def arrange_bins(me, raw, near, far):
    row = lax.broadcasted_iota(jnp.int32, (128, 128), 0)
    lane = lax.broadcasted_iota(jnp.int32, (128, 128), 1)
    rcol, rky2 = row % 32, row // 32
    lcol, lky2 = lane % 4, lane // 4
    low = me < 64
    wanted = []
    for t in range(4):
        slot = 4 * t + lcol
        own, other = slot, 32 - slot
        if t == 0:
            own = jnp.where(slot == 0, jnp.where(low, 16, 0), own)
            other = jnp.where(slot == 0, jnp.where(low, 0, 16), other)
        wanted.append((rcol == own, lky2 - rky2))
        wanted.append((rcol == other, 31 - lky2 - rky2))
    wanted.append((jnp.logical_and(lcol == 0, rcol == 0), lky2 - rky2))
    sums = [jnp.zeros((128, 128), F32) for _ in wanted]
    for g in range(8):
        pieces = [raw[:, pl.ds((4 * g + i) * 128, 128)].astype(F32) for i in range(4)]
        data = jnp.concatenate(pieces, axis=0).T.astype(BF16)
        for i, (match, shift) in enumerate(wanted):
            pick = jnp.where(jnp.logical_and(match, shift == 4 * g), 1.0, 0.0).astype(BF16)
            sums[i] = sums[i] + jnp.dot(data, pick, preferred_element_type=F32)
    flip = jnp.where(jnp.logical_and(row + lane == 128, row > 0), 1.0, 0.0).astype(BF16)
    for t in range(4):
        own, other = sums[2 * t], sums[2 * t + 1]
        if t == 0:
            own = jnp.where(jnp.logical_and(lcol == 0, me == 64), float(NBINS), own)
        near[t] = own
        turned = jnp.dot(flip, other.astype(BF16), preferred_element_type=F32)
        first = jnp.concatenate([other[:1, 124:], other[:1, :124]], axis=1)
        far[t] = jnp.where(row == 0, first, turned)
    near[4] = sums[8]


def bin_power(near, far, power, acc, spec):
    def group(g, _):
        sums = [jnp.zeros((8, 128), F32) for _ in range(8)]
        for i in range(9):
            t = i % 5 if i < 5 else i - 5
            which = 0 if i < 5 else 1
            for r in range(16):
                at = pl.ds(r * 8, 8)
                b = (far if which else near)[t, at, :] - (g * 8).astype(F32)
                p = power[t, at, :]
                for k in range(8):
                    sums[k] = sums[k] + jnp.where(b == float(k), p, 0.0)
        rows = [jnp.sum(v, axis=0, keepdims=True) for v in sums]
        acc[pl.ds(pl.multiple_of(g * 8, 8), 8), :] = jnp.concatenate(rows, axis=0)
        return 0

    lax.fori_loop(0, 8, group, 0)
    acc[pl.ds(64, 64), :] = jnp.zeros((64, 128), F32)
    row = jnp.sum(acc[...].T, axis=0, keepdims=True)
    spec[0] = row * (NBINS / float(N) ** 4)


class Reduction:
    def __init__(self, spread, total, yrelay, ydirect, yfinal, zrecv, zsum, ssem, rsem):
        self.spread, self.total, self.zrecv, self.zsum = spread, total, zrecv, zsum
        self.yrelay, self.ydirect, self.yfinal = yrelay, ydirect, yfinal
        self.ssem, self.rsem, self.sends = ssem, rsem, []
        y, zh = lax.axis_index("y"), lax.axis_index("zh")
        base = my_index() - y * 2 - zh
        up, down, across = lax.rem(y + 1, 4), lax.rem(y + 3, 4), lax.rem(y + 2, 4)
        self.y, self.zh, self.turn = y, zh, (across, up, down, y)
        self.dev_up, self.dev_down = base + up * 2 + zh, base + down * 2 + zh
        self.dev_z = base + y * 2 + (1 - zh)
        self.moves = {}

    def send(self, key, src, dst, to):
        i = len(self.sends)
        copy = pltpu.make_async_remote_copy(
            src_ref=src,
            dst_ref=dst,
            send_sem=self.ssem.at[i],
            recv_sem=self.rsem.at[i],
            device_id=to,
            device_id_type=LOGICAL,
        )
        copy.start()
        self.sends.append(copy)
        self.moves[key] = copy

    def arrived(self, *keys):
        for key in keys:
            self.moves[key].wait_recv()

    def share(self, t, h, b):
        return self.spread.at[pl.ds(pl.multiple_of(b * 1024 + (t * 2 + h) * 128, 128), 128)]


    def y_start(self, b):
        across, up, down, _ = self.turn
        self.send(("relay", b, 0), self.share(across, 0, b), self.yrelay.at[b, 0], self.dev_up)
        self.send(("relay", b, 1), self.share(across, 1, b), self.yrelay.at[b, 1], self.dev_down)
        self.send(("direct", b, 0), self.share(up, 1, b), self.ydirect.at[b, 1], self.dev_up)
        self.send(("direct", b, 1), self.share(down, 0, b), self.ydirect.at[b, 0], self.dev_down)

    def y_relay(self, b):
        for h, t, to in ((0, self.turn[1], self.dev_up), (1, self.turn[2], self.dev_down)):
            self.arrived(("relay", b, h))
            self.yrelay[b, h] = self.yrelay[b, h] + self.share(t, h, b)[...]
            self.send(("final", b, h), self.yrelay.at[b, h], self.yfinal.at[b, h], to)

    def y_finish(self, b):
        self.arrived(("direct", b, 0), ("direct", b, 1), ("final", b, 0), ("final", b, 1))
        for h in range(2):
            own = self.share(self.y, h, b)[...]
            self.yfinal[b, h] = self.yfinal[b, h] + self.ydirect[b, h] + own
        self.send(("z", b, 0), self.yfinal.at[b, 1 - self.zh], self.zrecv.at[b, 0], self.dev_z)

    def z_last(self, b):
        self.arrived(("z", b, 0))
        self.total[b] = self.zrecv[b, 0] + self.yfinal[b, self.zh]


    def z_start(self, b):
        for i, t in enumerate(self.turn):
            self.send(("z", b, i), self.share(t, 1 - self.zh, b), self.zrecv.at[b, i], self.dev_z)

    def z_then_y(self, b):
        low, high = pl.ds(0, 64), pl.ds(64, 64)
        zsum = self.zsum
        for i, t in enumerate(self.turn):
            self.arrived(("z", b, i))
            zsum[b, i] = self.zrecv[b, i] + self.share(t, self.zh, b)[...]
            if i == 0:
                up, down = self.yrelay.at[b, 0, low], self.yrelay.at[b, 1, low]
                self.send(("relay", b, 0), zsum.at[b, 0, low], up, self.dev_up)
                self.send(("relay", b, 1), zsum.at[b, 0, high], down, self.dev_down)
            if i == 1:
                up = self.ydirect.at[b, 1, low]
                self.send(("direct", b, 0), zsum.at[b, 1, high], up, self.dev_up)
            if i == 2:
                down = self.ydirect.at[b, 0, low]
                self.send(("direct", b, 1), zsum.at[b, 2, low], down, self.dev_down)

    def y_relay_half(self, b):
        low = pl.ds(0, 64)
        for h, i, to in ((0, 1, self.dev_up), (1, 2, self.dev_down)):
            self.arrived(("relay", b, h))
            own = self.zsum[b, i, pl.ds(h * 64, 64)]
            self.yrelay[b, h, low] = self.yrelay[b, h, low] + own
            self.send(("final", b, h), self.yrelay.at[b, h, low], self.yfinal.at[b, h, low], to)

    def y_last(self, b):
        self.arrived(("direct", b, 0), ("direct", b, 1), ("final", b, 0), ("final", b, 1))
        low = pl.ds(0, 64)
        for h in range(2):
            rows = pl.ds(h * 64, 64)
            new = self.yfinal[b, h, low] + self.ydirect[b, h, low]
            self.total[b, rows] = self.zsum[b, 3, rows] + new


def kernel(
    density, weight, bins_in, mats_in, out_real, out_imag, out_spec,
    recvc, specs, ctw, rtw, mine, spread, total, mats, yrelay, ydirect, yfinal, zrecv, zsum,
    ubuf, recvb, msgc, power, acc, spec, raw, near, far, farin, extra,
    lsem, msem, bsem, fsem, ssem, rsem, asem,
):
    me = my_index()
    barrier = pltpu.get_barrier_semaphore()
    mload = pltpu.make_async_copy(mats_in, mats, msem)
    mload.start()
    loads = {}
    for i in (5, 0, 6, 1, 7, 2, 3, 4):
        copy = pltpu.make_async_copy(
            density.at[0, pl.ds(i * 32, 32)], mine.at[pl.ds(i * 32, 32)], lsem.at[i]
        )
        copy.start()
        loads[i] = copy
    bload = pltpu.make_async_copy(bins_in, raw, bsem)
    bload.start()

    def greet(i, _):
        pl.semaphore_signal(
            barrier, inc=1, device_id=lax.rem(me + i, DEVICES), device_id_type=LOGICAL
        )
        return 0

    lax.fori_loop(1, DEVICES, greet, 0)
    w = weight[0]
    mload.wait()
    read_twiddles(mats, ctw, rtw)
    row, plane = me // 8, lax.rem(me, 8)
    red = Reduction(spread, total, yrelay, ydirect, yfinal, zrecv, zsum, ssem, rsem)

    def transform(b):
        loads[b].wait()
        row_forward(b, w, mine, mats, rtw, ubuf, spread)

    def to_columns(b):
        at = pl.ds(pl.multiple_of((row * 8 + b) * 8, 8), 8)

        def step(i, _):
            to = lax.rem(row + i * 5, 16)
            pltpu.make_async_remote_copy(
                src_ref=total.at[b, pl.ds(pl.multiple_of(to * 8, 8), 8)],
                dst_ref=recvb.at[at],
                send_sem=asem.at[0],
                recv_sem=asem.at[1],
                device_id=to * 8 + plane,
                device_id_type=LOGICAL,
            ).start()
            return 0

        lax.fori_loop(1, 16, step, 0)
        recvb[at, :] = total[b, pl.ds(pl.multiple_of(row * 8, 8), 8), :]

    transform(5)
    transform(0)
    pl.semaphore_wait(barrier, DEVICES - 1)
    red.z_start(5)
    red.y_start(0)
    transform(6)
    red.z_start(6)
    transform(1)
    red.y_start(1)
    red.y_relay(0)
    transform(7)
    red.z_start(7)
    transform(2)
    red.y_start(2)
    red.y_relay(1)
    transform(3)
    transform(4)
    red.z_then_y(5)
    red.y_start(3)
    red.y_relay(2)
    red.y_finish(0)
    red.y_relay_half(5)
    bload.wait()
    arrange_bins(me, raw, near, far)
    red.y_start(4)
    red.y_relay(3)
    red.y_finish(1)
    red.z_then_y(6)
    red.y_relay(4)
    red.y_relay_half(6)
    red.y_finish(2)
    red.y_last(5)
    to_columns(5)
    red.z_last(0)
    to_columns(0)
    red.y_finish(3)
    red.z_then_y(7)
    red.z_last(1)
    to_columns(1)
    red.y_relay_half(7)
    red.y_finish(4)
    red.y_last(6)
    to_columns(6)
    red.z_last(2)
    to_columns(2)
    red.z_last(3)
    to_columns(3)
    red.y_last(7)
    to_columns(7)
    red.z_last(4)
    to_columns(4)
    mirror = pltpu.make_async_remote_copy(
        src_ref=far,
        dst_ref=farin,
        send_sem=fsem.at[0],
        recv_sem=fsem.at[1],
        device_id=DEVICES - 1 - me,
        device_id_type=LOGICAL,
    )
    mirror.start()
    zeroth = pltpu.make_async_remote_copy(
        src_ref=far.at[0],
        dst_ref=extra,
        send_sem=fsem.at[2],
        recv_sem=fsem.at[3],
        device_id=jnp.where(me == 0, 64, DEVICES - me),
        device_id_type=LOGICAL,
    )

    @pl.when(me < 64)
    def _():
        zeroth.start()

    wait_all(recvb, asem.at[1], 8, 120)

    def to_rows(ac):
        send_all(me, ac, msgc, recvc, asem.at[2 + ac], asem.at[6 + ac])

    column_part(me, recvb, mats, ctw, power, msgc, to_rows)
    mirror.wait_recv()

    @pl.when(me >= 64)
    def _():
        zeroth.wait_recv()
        lane = lax.broadcasted_iota(jnp.int32, (128, 128), 1)
        farin[0] = jnp.where(lane % 4 == 0, extra[...], farin[0])

    bin_power(near, farin, power, acc, spec)

    def share_spec(i, _):
        to = peer(me, i)
        pltpu.make_async_remote_copy(
            src_ref=spec.at[0],
            dst_ref=specs.at[me],
            send_sem=asem.at[4],
            recv_sem=asem.at[5],
            device_id=to,
            device_id_type=LOGICAL,
        ).start()
        return 0

    lax.fori_loop(1, DEVICES, share_spec, 0)
    specs[me] = spec[0]
    wait_all(recvc, asem.at[6], 8)
    row_inverse(0, recvc, mats, rtw, ubuf, out_real)
    wait_all(recvc, asem.at[7], 8)
    row_inverse(1, recvc, mats, rtw, ubuf, out_imag)
    wait_all(specs, asem.at[5], 1)
    power_sum = specs[0]
    for i in range(1, DEVICES):
        power_sum = power_sum + specs[i]
    out_spec[...] = power_sum[:, :NBINS]
    wait_all(recvb, asem.at[0], 8, 120)
    wait_all(msgc, asem.at[2], 8)
    wait_all(msgc, asem.at[3], 8)
    wait_all(specs, asem.at[4], 1)
    for copy in red.sends:
        copy.wait_send()
    mirror.wait_send()

    @pl.when(me < 64)
    def _():
        zeroth.wait_send()


def finish(*refs):
    sems = refs[6]
    copies = [pltpu.make_async_copy(refs[i], refs[3 + i], sems.at[i]) for i in range(3)]
    for copy in copies:
        copy.start()
    for copy in copies:
        copy.wait()


def on_device(mats, density, lens_weight, spectrum_bin):
    vmem = pl.BlockSpec(memory_space=pltpu.VMEM)
    hbm = pl.BlockSpec(memory_space=pltpu.HBM)
    smem = pl.BlockSpec(memory_space=pltpu.SMEM)
    dma = pltpu.SemaphoreType.DMA
    share = (128, 128)
    params = partial(pltpu.CompilerParams, vmem_limit_bytes=55050240)
    shapes = (
        jax.ShapeDtypeStruct((32, N), F32),
        jax.ShapeDtypeStruct((32, N), F32),
        jax.ShapeDtypeStruct((1, NBINS), F32),
    )
    results = pl.pallas_call(
        kernel,
        name="shear",
        out_shape=shapes,
        in_specs=[hbm, smem, hbm, hbm],
        out_specs=(vmem, vmem, vmem),
        scratch_shapes=[
            pltpu.VMEM((DEVICES * 16, 128), F32),
            pltpu.VMEM((DEVICES, 1, 128), F32),
            pltpu.VMEM((2, 128, 128), F32),
            pltpu.VMEM((2, 16, 128), F32),
            pltpu.VMEM((256, N), F32),
            pltpu.VMEM((8 * 1024, 128), F32),
            pltpu.VMEM((8,) + share, F32),
            pltpu.VMEM((7, 2, 256, 256), BF16),
            pltpu.VMEM((8, 2) + share, F32),
            pltpu.VMEM((8, 2) + share, F32),
            pltpu.VMEM((8, 2) + share, F32),
            pltpu.VMEM((8, 4) + share, F32),
            pltpu.VMEM((8, 4) + share, F32),
            pltpu.VMEM((2, 512, 128), F32),
            pltpu.VMEM((DEVICES * 8, 128), F32),
            pltpu.VMEM((DEVICES * 16, 128), F32),
            pltpu.VMEM((5, 128, 128), F32),
            pltpu.VMEM((128, 128), F32),
            pltpu.VMEM((1, 1, 128), F32),
            pltpu.VMEM((32, N), jnp.int32),
            pltpu.VMEM((5, 128, 128), F32),
            pltpu.VMEM((4, 128, 128), F32),
            pltpu.VMEM((4, 128, 128), F32),
            pltpu.VMEM((128, 128), F32),
            dma((8,)),
            dma,
            dma,
            dma((4,)),
            dma((80,)),
            dma((80,)),
            dma((8,)),
        ],
        compiler_params=params(collective_id=0, has_side_effects=True),
    )(density, lens_weight, spectrum_bin.T, mats)
    real, imag, spectrum = pl.pallas_call(
        finish,
        name="finish",
        out_shape=shapes,
        in_specs=[vmem, vmem, vmem],
        out_specs=(hbm, hbm, hbm),
        scratch_shapes=[dma((3,))],
        compiler_params=params(),
    )(*results)
    return real, imag, spectrum.reshape(NBINS)


def solution(mesh):
    finer = Mesh(mesh.devices.reshape(4, 2, 2, 4, 2), AXES)
    tables = jnp.asarray(make_tables())
    step = jax.shard_map(
        on_device,
        mesh=finer,
        in_specs=(P(), P(PLANES, ROWS, None), P(PLANES), P(None, AXES)),
        out_specs=(P(AXES, None), P(AXES, None), P()),
        check_vma=False,
    )

    def whole(density, lens_weight, spectrum_bin):
        return step(tables, density, lens_weight, spectrum_bin)

    return whole
```
